32 devices in a mesh: sub: 8 (over z, x), grp: 4 (over y, core).
Axes of the slice: x: 2, y: 2, z: 4, core: 2. Of those that a mesh axis runs over, the one named last changes fastest.
Arguments:
- solution: float32 [32, 128, 2048], P(('sub', 'grp')), may hold values from -6 to 6
- residual: float32 [32, 128, 2048], P(('sub', 'grp'))
- direction: float32 [32, 128, 2048], P(('sub', 'grp'))
- residual_product: float32 [128], replicated, may hold values from 65536 to 1310720
- neighbor_slots: int32 [32, 4], P(('sub', 'grp')), may hold values from 0 to 3, each once within a row
- coupling: bfloat16 [32, 96, 256, 128], P(('sub', 'grp')), may hold values from -0.375 to 0.375
- dirichlet_factor: bfloat16 [32, 96, 128, 128], P(('sub', 'grp')), may hold values from -0.5 to 0.5
- face_block: bfloat16 [32, 32, 128, 128], P(('sub', 'grp')), as said below
- neumann_factor: bfloat16 [32, 32, 128, 128], P(('sub', 'grp')), may hold values from -0.5 to 0.5
- primal_block: int32 [32, 128], P(('sub', 'grp')), may hold values from 0 to 31
- primal_basis: bfloat16 [32, 128, 128], P(('sub', 'grp')), may hold values from -1.5 to 1.5
- coarse_matrix: float32 [32, 9, 128, 128], P(('sub', 'grp')), may hold values from -0.17677669 to 0.17677669
- coarse_block_inverse: float32 [32, 128, 128], P(('sub', 'grp')), may hold values from -0.5 to 0.5
- coarse_pattern: int32 [32, 9], P(('sub', 'grp')), may hold values from 0 to 31, as said below
Outputs:
- new_solution: float32 [32, 128, 2048], P(('sub', 'grp'))
- new_residual: float32 [32, 128, 2048], P(('sub', 'grp'))
- new_direction: float32 [32, 128, 2048], P(('sub', 'grp'))
- new_product: float32 [128], replicated
The draws below stay inside these ranges and needn't reach their ends.
Inputs may be any that keep to these rules, and one draw needn't show every extreme that they name: `neighbor_slots`: each row orders the four local face slots: entry d is the slot of the face toward direction d (sub lower, sub upper, grp lower, grp upper). `coarse_pattern`: row t names 9 different subdomains, the first of them t itself; subdomain s lies on the device of index s along sub+grp, and every entry lies within 2 positions of row t along sub, cyclically. `face_block`: each block is symmetric with every eigenvalue at least 0.5.
All inputs are finite; a program needn't handle non-finite values.
Results may differ from the reference program's by a relative error of at most 0.0003.
Values sent between devices are 32-bit elements; how exact they have to be, the bound alone decides.
No kernel may reach another device: no remote copies, remote signals or barrier semaphores. Data moves between devices by JAX's collectives and lax.ppermute only.
A program may use at most 128 MiB of HBM per device.

```python
import math
import jax
import jax.numpy as jnp
from jax import lax

LOAD_CASES = 128
FACE_SIZE = 1024
BLOCK_SIZE = 128
PRIMALS = 128
PATTERN_BLOCKS = 9
REACH_SUBS = 2
FACE_BLOCKS = 32
INNER_BLOCKS = 96
SUBDOMAINS = 32
N_SUB = 8
N_GRP = 4


def ramped_field(key, salt):
    full_shape = (SUBDOMAINS, LOAD_CASES, 2 * FACE_SIZE)
    base_key = jax.random.fold_in(key, salt)
    column = jnp.exp(jax.random.uniform(jax.random.fold_in(base_key, 1), (1, 1, 2 * FACE_SIZE), jnp.float32, math.log(0.3), math.log(3.0)))
    across = jnp.exp(jax.random.uniform(jax.random.fold_in(base_key, 2), (1, LOAD_CASES, 1), jnp.float32, math.log(0.6), math.log(2.0)))
    position = jnp.arange(SUBDOMAINS, dtype=jnp.float32) / (SUBDOMAINS - 1)
    values = jax.random.normal(jax.random.fold_in(base_key, 3), full_shape, jnp.float32)
    ramp_scale = jnp.exp(math.log(3.0) * position)
    return values * column * across * ramp_scale[:, None, None]


def draw_residual(key, part):
    return ramped_field(key, 11)


def draw_direction(key, part):
    return ramped_field(key, 23)


def draw_face_block(key, part):
    full_shape = (SUBDOMAINS, FACE_BLOCKS, BLOCK_SIZE, BLOCK_SIZE)
    mixing = jax.random.normal(jax.random.fold_in(key, 31), full_shape, jnp.float32)
    gram_part = jnp.einsum('sjab,sjcb->sjac', mixing, mixing) / BLOCK_SIZE
    low_end = 0.5
    high_end = 2.0
    diagonal = jnp.exp(jax.random.uniform(jax.random.fold_in(key, 32), full_shape[:3], jnp.float32, math.log(low_end), math.log(high_end)))
    return (gram_part + diagonal[..., None] * jnp.eye(BLOCK_SIZE, dtype=jnp.float32)).astype(jnp.bfloat16)


def draw_coarse_pattern(key, part):
    candidates = N_GRP * (2 * REACH_SUBS + 1) - 1
    row_ids = jnp.arange(SUBDOMAINS, dtype=jnp.int32)

    def one_row(row_id):
        shuffled = jax.random.permutation(jax.random.fold_in(jax.random.fold_in(key, 41), row_id), candidates)
        chosen = shuffled[:PATTERN_BLOCKS - 1].astype(jnp.int32)
        own_slot = REACH_SUBS * N_GRP + row_id % N_GRP
        chosen = chosen + (chosen >= own_slot).astype(jnp.int32)
        entry_sub = (row_id // N_GRP + chosen // N_GRP - REACH_SUBS) % N_SUB
        entries = entry_sub * N_GRP + chosen % N_GRP
        return jnp.concatenate([row_id[None], entries]).astype(jnp.int32)
    return jax.vmap(one_row)(row_ids)


def plant(values, key, least, largest):
    place = [jax.random.randint(jax.random.fold_in(key, axis), (), 0, length) for axis, length in enumerate(values.shape)]
    longest = values.shape.index(max(values.shape))
    beside = place[:longest] + [(place[longest] + 1) % values.shape[longest]] + place[longest + 1:]
    return values.at[tuple(place)].set(least).at[tuple(beside)].set(largest)


def level_of(rng, extent, pieces, least, largest):
    def one(dim, blocks):
        draws = jax.random.uniform(jax.random.fold_in(jax.random.fold_in(rng, 6), dim), (blocks,), jnp.float32, least / len(pieces), largest / len(pieces))
        return jnp.repeat(jnp.exp(draws), extent[dim] // blocks).reshape((-1,) + (1,) * (len(extent) - dim - 1))

    loudness = one(*pieces[0])
    for cut in pieces[1:]:
        loudness = loudness * one(*cut)
    return loudness


def noise(own_key, extent, width, bound, cuts=(), kind=jnp.bfloat16):
    values = jax.random.normal(own_key, extent, jnp.float32) * width
    if len(cuts) > 0:
        values = level_of(own_key, extent, cuts, -0.22, 0.18) * values
    return jnp.clip(values, min=-bound, max=bound).astype(kind)


def setup_inputs(seed: int = 0) -> dict:
    arg_keys = jax.random.split(jax.random.key(seed), 15)
    return {
        "solution": noise(arg_keys[0], (SUBDOMAINS, LOAD_CASES, 2 * FACE_SIZE), 1.0, 6.0, ((0, 32),), jnp.float32),
        "residual": draw_residual(jax.random.fold_in(arg_keys[14], 71), 0),
        "direction": draw_direction(jax.random.fold_in(arg_keys[14], 71), 0),
        "residual_product": jnp.clip(jnp.exp(jax.random.uniform(arg_keys[3], (LOAD_CASES,), jnp.float32, math.log(65536.0), math.log(1310720))), 65536.0, 1310720),
        "neighbor_slots": jax.vmap(lambda own: jax.random.permutation(own, 4))(jax.random.split(arg_keys[4], SUBDOMAINS)).reshape((SUBDOMAINS, 4)).astype(jnp.int32),
        "coupling": noise(arg_keys[5], (SUBDOMAINS, INNER_BLOCKS, 2 * BLOCK_SIZE, BLOCK_SIZE), (2 * BLOCK_SIZE) ** -0.5, 0.375, ((0, 32),)),
        "dirichlet_factor": noise(arg_keys[6], (SUBDOMAINS, INNER_BLOCKS, BLOCK_SIZE, BLOCK_SIZE), BLOCK_SIZE ** -0.5, 0.5, ((0, 32),)),
        "face_block": draw_face_block(jax.random.fold_in(arg_keys[14], 71), 0),
        "neumann_factor": noise(arg_keys[8], (SUBDOMAINS, FACE_BLOCKS, BLOCK_SIZE, BLOCK_SIZE), BLOCK_SIZE ** -0.5, 0.5, ((0, 32),)),
        "primal_block": plant(jax.random.randint(arg_keys[9], (SUBDOMAINS, PRIMALS), 0, FACE_BLOCKS), jax.random.fold_in(arg_keys[9], 1), 0, FACE_BLOCKS - 1).astype(jnp.int32),
        "primal_basis": noise(arg_keys[10], (SUBDOMAINS, PRIMALS, BLOCK_SIZE), (BLOCK_SIZE // 8) ** -0.5, 1.5, ((0, 32),)),
        "coarse_matrix": noise(arg_keys[11], (SUBDOMAINS, PATTERN_BLOCKS, PRIMALS, PRIMALS), (1.0 / (PATTERN_BLOCKS * PRIMALS) ** 0.5), 0.17677669, ((0, 32),), jnp.float32),
        "coarse_block_inverse": noise(arg_keys[12], (SUBDOMAINS, PRIMALS, PRIMALS), PRIMALS ** -0.5, 0.5, ((0, 32),), jnp.float32),
        "coarse_pattern": draw_coarse_pattern(jax.random.fold_in(arg_keys[14], 71), 0),
    }


highest_precision = lax.Precision.HIGHEST


def onehot_slots(neighbor_slots):
    return (neighbor_slots[:, :, None] == jnp.arange(4, dtype=jnp.int32)[None, None, :]).astype(jnp.float32)


def spread(owned_part, slot_onehot):
    face_width = owned_part.shape[2] // 2
    load_count = owned_part.shape[1]
    own_sub = owned_part[:, :, :face_width].reshape(N_SUB, N_GRP, load_count, face_width)
    own_grp = owned_part[:, :, face_width:].reshape(N_SUB, N_GRP, load_count, face_width)
    from_sub = jnp.roll(own_sub, 1, axis=0)
    from_grp = jnp.roll(own_grp, 1, axis=1)
    directed = jnp.stack([from_sub, own_sub, from_grp, own_grp], 2).reshape(SUBDOMAINS, 4, load_count, face_width)
    placed = jnp.einsum('sdk,sdlf->slkf', slot_onehot, directed, precision=highest_precision)
    return placed.reshape(SUBDOMAINS, load_count, FACE_BLOCKS, BLOCK_SIZE)


def collect(local_part, slot_onehot):
    load_count = local_part.shape[1]
    placed = local_part.reshape(SUBDOMAINS, load_count, 4, FACE_SIZE)
    directed = jnp.einsum('sdk,slkf->sdlf', slot_onehot, placed, precision=highest_precision)
    grid_form = directed.reshape(N_SUB, N_GRP, 4, load_count, FACE_SIZE)
    owned_sub = grid_form[:, :, 1] + jnp.roll(grid_form[:, :, 0], -1, axis=0)
    owned_grp = grid_form[:, :, 3] + jnp.roll(grid_form[:, :, 2], -1, axis=1)
    return jnp.concatenate([owned_sub, owned_grp], 3).reshape(SUBDOMAINS, load_count, 2 * FACE_SIZE)


def condensed(vector, couple, dirichlet, face_matrix):
    count_of_blocks = vector.shape[1]
    block_width = vector.shape[2]
    paired = jnp.concatenate([jnp.concatenate([vector, jnp.roll(vector, -(offset + 1), axis=1)], 2) for offset in range(3)], 1)
    interior = jnp.einsum('lib,ibk->lik', paired, couple, precision=highest_precision)
    middle = jnp.einsum('lik,ikm->lim', interior, dirichlet, precision=highest_precision)
    solved = jnp.einsum('lim,ikm->lik', middle, dirichlet, precision=highest_precision)
    returned = jnp.einsum('lik,ibk->lib', solved, couple, precision=highest_precision)
    result = jnp.einsum('ljb,jbk->ljk', vector, face_matrix, precision=highest_precision)
    for offset in range(3):
        portion = returned[:, offset * count_of_blocks:(offset + 1) * count_of_blocks]
        result = result + portion[:, :, :block_width] + jnp.roll(portion[:, :, block_width:], offset + 1, axis=1)
    return result


def apply_condensed(operands):
    vector, couple, dirichlet, face_matrix = operands
    return condensed(vector, couple.astype(jnp.float32), dirichlet.astype(jnp.float32), face_matrix.astype(jnp.float32))


def local_precondition(operands):
    halved, neumann, block_ids, basis = operands
    neumann = neumann.astype(jnp.float32)
    basis = basis.astype(jnp.float32)
    neumann_step = jnp.einsum('ljb,jbk->ljk', halved, neumann, precision=highest_precision)
    local_solve = jnp.einsum('ljk,jmk->ljm', neumann_step, neumann, precision=highest_precision)
    selector = (block_ids[:, None] == jnp.arange(halved.shape[1], dtype=jnp.int32)[None, :]).astype(jnp.float32)
    picked = jnp.einsum('ljb,cj->lcb', halved, selector, precision=highest_precision)
    coarse_residual = jnp.einsum('lcb,cb->lc', picked, basis, precision=highest_precision)
    return local_solve, coarse_residual


def spread_coarse(operands):
    coarse_correction, block_ids, basis = operands
    basis = basis.astype(jnp.float32)
    selector = (block_ids[:, None] == jnp.arange(FACE_BLOCKS, dtype=jnp.int32)[None, :]).astype(jnp.float32)
    weighted = coarse_correction[:, :, None] * basis[None]
    return jnp.einsum('lcb,cj->ljb', weighted, selector, precision=highest_precision)


def precondition(owned_part, slot_onehot, neumann_factor, primal_block, primal_basis, coarse_matrix, coarse_block_inverse, coarse_pattern):
    halved = spread(owned_part, slot_onehot) * 0.5
    local_solve, coarse_residual = lax.map(local_precondition, (halved, neumann_factor, primal_block, primal_basis))
    initial_step = jnp.einsum('pqe,pek->pqk', coarse_residual, coarse_block_inverse, precision=highest_precision)
    gathered = initial_step[coarse_pattern]
    adjacent_sum = jnp.einsum('skld,skde->sle', gathered, coarse_matrix, precision=highest_precision)
    coarse_correction = initial_step + jnp.einsum('iqc,icw->iqw', coarse_residual - adjacent_sum, coarse_block_inverse, precision=highest_precision)
    spread_back = lax.map(spread_coarse, (coarse_correction, primal_block, primal_basis))
    return collect(0.5 * (local_solve + spread_back), slot_onehot)


def reference(solution, residual, direction, residual_product, neighbor_slots, coupling, dirichlet_factor, face_block, neumann_factor, primal_block, primal_basis, coarse_matrix, coarse_block_inverse, coarse_pattern):
    slot_onehot = onehot_slots(neighbor_slots)
    local_image = lax.map(apply_condensed, (spread(direction, slot_onehot), coupling, dirichlet_factor, face_block))
    image = collect(local_image, slot_onehot)
    curvature = jnp.sum(direction * image, axis=(0, 2))
    step_length = residual_product / curvature
    new_solution = solution + step_length[None, :, None] * direction
    new_residual = residual - step_length[None, :, None] * image
    preconditioned = precondition(new_residual, slot_onehot, neumann_factor, primal_block, primal_basis, coarse_matrix, coarse_block_inverse, coarse_pattern)
    new_product = jnp.sum(new_residual * preconditioned, axis=(0, 2))
    step_ratio = new_product / residual_product
    new_direction = preconditioned + step_ratio[None, :, None] * direction
    return new_solution, new_residual, new_direction, new_product
```

```python
import functools

import jax
import jax.numpy as jnp
from jax import lax
from jax.experimental import pallas as pl
from jax.experimental.pallas import tpu as pltpu
from jax.sharding import PartitionSpec as P

REACH_SUBS = 2
F32 = jnp.float32
BF16 = jnp.bfloat16
VMEM = pl.BlockSpec(memory_space=pltpu.VMEM)
SMEM = pl.BlockSpec(memory_space=pltpu.SMEM)
NN = (((1,), (0,)), ((), ()))
NT = (((1,), (1,)), ((), ()))


def shifted(value, axis, steps):
    count = lax.axis_size(axis)
    pairs = [(source, (source + steps) % count) for source in range(count)]
    return lax.ppermute(value, axis, pairs)


def total(value, axis):
    count = lax.axis_size(axis)
    if count & (count - 1):
        return lax.psum(value, axis)
    bit = 1
    while bit < count:
        value = value + lax.ppermute(value, axis, [(i, i ^ bit) for i in range(count)])
        bit *= 2
    return value


def grand_total(value):
    return total(total(value, "grp"), "sub")


def split(value):
    high = value.astype(BF16)
    low = (value - high.astype(F32)).astype(BF16)
    return high, low


def mm(a, b, dims=NN):
    return lax.dot_general(a, b, dims, preferred_element_type=F32)


def mm3(a, b):
    a_high, a_low = split(a)
    b_high, b_low = split(b)
    return mm(a_high, b_high) + (mm(a_low, b_high) + mm(a_high, b_low))


def twice(value, axis):
    return jnp.concatenate([value, value], axis=axis)


def row_sums(partial):
    ones = jnp.ones((8, partial.shape[1]), F32)
    return lax.dot_general(ones, partial, NT, precision=lax.Precision.HIGHEST, preferred_element_type=F32)


def per_row(row, width):
    tall = jnp.broadcast_to(row[0:1], (width, row.shape[1]))
    return tall.T


def call(body, out_shapes, name, flops, moved, scratch=(), grid=None, in_specs=None, out_specs=None, limit=None):
    params = {}
    if limit is not None:
        params["vmem_limit_bytes"] = limit
    kwargs = {}
    if grid is not None:
        kwargs["grid"] = grid
    return pl.pallas_call(
        body,
        out_shape=out_shapes,
        in_specs=in_specs,
        out_specs=out_specs,
        scratch_shapes=scratch,
        compiler_params=pltpu.CompilerParams(**params),
        cost_estimate=pl.CostEstimate(flops=flops, bytes_accessed=moved, transcendentals=0),
        name=name,
        **kwargs,
    )


def assemble_body(blocks, couple_ref, dirichlet_ref, face_ref, high_ref, low_ref, diag_ref):
    step = pl.program_id(0)
    pairs = blocks // 2
    width = face_ref.shape[1]
    reach = couple_ref.shape[0]

    @pl.when(step == 0)
    def _():
        diag_ref[...] = face_ref[...].astype(F32)

    def put(pair, row, half, value):
        high, low = split(value)
        rows = pl.ds(row * width, width)
        cols = pl.ds(half * width, width)
        high_ref[pair, rows, cols] = high
        low_ref[pair, rows, cols] = low

    zero = jnp.zeros((width, width), BF16)
    for ref in (high_ref, low_ref):
        ref[step, pl.ds((2 * reach + 1) * width, width), pl.ds(0, width)] = zero
        ref[step, pl.ds(0, width), pl.ds(width, width)] = zero
    own = [0.0, 0.0]
    for side in range(2):
        own_sum = None
        for q in range(reach):
            couple = couple_ref[q, side]
            factor = dirichlet_ref[q, side]
            inner_high, inner_low = split(mm(factor, factor, NT))
            middle = mm(twice(couple, 1), jnp.concatenate([inner_high, inner_low], 0))
            middle_high, middle_low = split(middle)
            full = mm(jnp.concatenate([middle_high, middle_low], 1), twice(couple, 1), NT)
            near = full[:width, :width]
            far = full[width:, width:]
            own_sum = near if own_sum is None else own_sum + near
            reached = side + q + 1
            half = reached % 2
            pair = lax.rem(step + reached // 2, pairs)
            put(pair, reach - (q + 1) + half, half, full[:width, width:])
            put(step, reach + (q + 1) + side, side, full[width:, :width])
            other = lax.rem(2 * step + reached, blocks)
            diag_ref[other] += far
        diag_ref[2 * step + side] += own_sum

    def finish(pair):
        for side in range(2):
            put(pair, reach + side, side, diag_ref[2 * pair + side])

    first = (reach + 1) // 2

    @pl.when(step >= first)
    def _():
        finish(step)

    @pl.when(step == pairs - 1)
    def _():
        for pair in range(first):
            finish(pair)


def assemble(coupling, dirichlet, face):
    blocks, width, _ = face.shape
    reach = coupling.shape[0] // blocks
    pairs = blocks // 2
    couple = coupling.reshape(reach, blocks, 2 * width, width)
    factor = dirichlet.reshape(reach, blocks, width, width)
    depth = (2 * reach + 2) * width
    shape = jax.ShapeDtypeStruct((pairs, depth, 2 * width), BF16)
    whole = pl.BlockSpec((pairs, depth, 2 * width), lambda i: (0, 0, 0))
    return call(
        functools.partial(assemble_body, blocks),
        (shape, shape),
        "assemble",
        flops=reach * blocks * 2 * width**3 * 12,
        moved=coupling.size * 3,
        scratch=[pltpu.VMEM((blocks, width, width), F32)],
        grid=(pairs,),
        in_specs=[
            pl.BlockSpec((reach, 2, 2 * width, width), lambda i: (0, i, 0, 0)),
            pl.BlockSpec((reach, 2, width, width), lambda i: (0, i, 0, 0)),
            pl.BlockSpec((blocks, width, width), lambda i: (0, 0, 0)),
        ],
        out_specs=(whole, whole),
        limit=ASSEMBLE_LIMIT,
    )(couple, factor, face)


ASSEMBLE_LIMIT = 28 * 1024 * 1024


def apply_body(slots_ref, own_ref, from_sub_ref, from_grp_ref, high_ref, low_ref, out_ref, curve_ref, u_high, u_low):
    step = pl.program_id(0)
    pairs = pl.num_programs(0)
    width = u_high.shape[2]
    face_width = from_sub_ref.shape[1]
    per_face = face_width // width
    blocks = 4 * per_face
    reach = (high_ref.shape[1] // width - 2) // 2

    def faces():
        own = own_ref
        return (
            lambda lo, n: from_sub_ref[:, lo : lo + n],
            lambda lo, n: own[:, lo : lo + n],
            lambda lo, n: from_grp_ref[:, lo : lo + n],
            lambda lo, n: own[:, face_width + lo : face_width + lo + n],
        )

    @pl.when(step == 0)
    def _():
        for which, face in enumerate(faces()):
            slot = slots_ref[0, which]
            for b in range(per_face):
                high, low = split(face(b * width, width))
                place = slot * per_face + b + reach
                u_high[place] = high
                u_low[place] = low
        for ref in (u_high, u_low):
            for i in range(reach):
                ref[i] = ref[blocks + i]
            for i in range(reach + 1):
                ref[blocks + reach + i] = ref[reach + i]

    count = 2 * reach + 2
    high = jnp.concatenate([u_high[2 * step + i] for i in range(count)], 1)
    low = jnp.concatenate([u_low[2 * step + i] for i in range(count)], 1)
    weight = high_ref[0]
    result = mm(high, weight) + mm(low, weight) + mm(high, low_ref[0])
    pair_slot = step // (per_face // 2)
    lane = pl.multiple_of((step - pair_slot * (per_face // 2)) * 2 * width, 2 * width)
    which = jnp.int32(0)
    for d in range(1, 4):
        which = jnp.where(slots_ref[0, d] == pair_slot, d, which)
    out_ref[which, :, pl.ds(lane, 2 * width)] = result

    @pl.when(step == pairs - 1)
    def _():
        acc = jnp.zeros((out_ref.shape[1], width), F32)
        for which, face in enumerate(faces()):
            for b in range(per_face):
                acc += face(b * width, width) * out_ref[which, :, b * width : (b + 1) * width]
        curve_ref[...] = row_sums(acc)


def apply(slots, own, from_sub, from_grp, high, low):
    pairs, depth, double = high.shape
    width = double // 2
    loads, face_width = from_sub.shape
    blocks = 2 * pairs
    reach = depth // width // 2 - 1
    block = pl.BlockSpec((1, depth, double), lambda i: (i, 0, 0))
    return call(
        apply_body,
        (
            jax.ShapeDtypeStruct((4, loads, face_width), F32),
            jax.ShapeDtypeStruct((8, loads), F32),
        ),
        "apply",
        flops=pairs * depth * double * loads * 6,
        moved=high.size * 4,
        scratch=[pltpu.VMEM((blocks + 2 * reach + 1, loads, width), BF16)] * 2,
        grid=(pairs,),
        in_specs=[
            SMEM,
            pl.BlockSpec(own.shape, lambda i: (0, 0)),
            pl.BlockSpec(from_sub.shape, lambda i: (0, 0)),
            pl.BlockSpec(from_grp.shape, lambda i: (0, 0)),
            block,
            block,
        ],
        out_specs=(
            pl.BlockSpec((4, loads, face_width), lambda i: (0, 0, 0)),
            pl.BlockSpec((8, loads), lambda i: (0, 0)),
        ),
        limit=20 * 1024 * 1024,
    )(slots, own, from_sub, from_grp, high, low)


def pack_body(per_face, slots_ref, block_ref, basis_ref, factor_ref, sub_ref, grp_ref):
    width = basis_ref.shape[1]
    rows = per_face * width
    prims = basis_ref.shape[0]
    for out, which in ((sub_ref, 0), (grp_ref, 2)):
        first = slots_ref[0, which] * per_face
        for b in range(per_face):
            out[b * width : (b + 1) * width, :] = factor_ref[first + b].astype(F32)
        out[rows : rows + prims, :] = basis_ref[...].astype(F32)
        near = (block_ref[...] - first).astype(F32)
        out[rows + prims :, :] = jnp.broadcast_to(near, (8, width))


def pack(slots, blocks, basis, factor, per_face):
    prims, width = basis.shape
    shape = jax.ShapeDtypeStruct((per_face * width + prims + 8, width), F32)
    return call(
        functools.partial(pack_body, per_face),
        (shape, shape),
        "pack",
        flops=1000,
        moved=shape.size * 12,
        in_specs=[SMEM, VMEM, VMEM, VMEM],
        out_specs=(VMEM, VMEM),
        limit=8 * 1024 * 1024,
    )(slots, blocks, basis, factor)


def update_body(slots_ref, y_ref, back_sub_ref, back_grp_ref, residual_ref, curve_ref, product_ref, block_ref, basis_ref, aux_sub_ref, aux_grp_ref, residual_out, own_out, sub_out, grp_out):
    width = basis_ref.shape[1]
    prims = basis_ref.shape[0]
    face_width = back_sub_ref.shape[1]
    per_face = face_width // width
    rows = face_width
    scale = per_row(product_ref[...] / curve_ref[...], width)
    basis = basis_ref[...].astype(F32).T
    own_total = None
    for which, back, aux, out in (
        (1, back_sub_ref, aux_sub_ref, sub_out),
        (3, back_grp_ref, aux_grp_ref, grp_out),
    ):
        offset = (which // 2) * face_width
        other = aux[rows : rows + prims, :].T
        own_near = block_ref[...] - slots_ref[0, which] * per_face
        other_near = aux[rows + prims : rows + prims + 1, :]
        lefts = []
        rights = []
        for b in range(per_face):
            cols = slice(b * width, (b + 1) * width)
            image = y_ref[which, :, cols] + back[:, cols]
            fresh = residual_ref[:, offset + b * width : offset + (b + 1) * width] - scale * image
            residual_out[:, offset + b * width : offset + (b + 1) * width] = fresh
            lefts.append(fresh * 0.5)
            mine = jnp.where(own_near == b, basis, 0.0).astype(BF16)
            theirs = jnp.where(other_near == b, other, 0.0).astype(BF16)
            rights.append(jnp.concatenate([mine, theirs], 1))
        high, low = split(jnp.concatenate(lefts, 1))
        right = jnp.concatenate(rights, 0)
        both = mm(high, right) + mm(low, right)
        own = both[:, :prims]
        own_total = own if own_total is None else own_total + own
        out[...] = both[:, prims:]
    own_out[...] = own_total


def update(slots, y, back_sub, back_grp, residual, curve, product, blocks, basis, aux_sub, aux_grp):
    loads = residual.shape[0]
    prims = basis.shape[0]
    small = jax.ShapeDtypeStruct((loads, prims), F32)
    return call(
        update_body,
        (jax.ShapeDtypeStruct(residual.shape, F32), small, small, small),
        "update",
        flops=residual.size * prims * 8,
        moved=residual.size * 20,
        in_specs=[SMEM] + [VMEM] * 10,
        out_specs=(VMEM,) * 4,
        limit=16 * 1024 * 1024,
    )(slots, y, back_sub, back_grp, residual, curve, product, blocks, basis, aux_sub, aux_grp)


def first_body(own_ref, sub_ref, grp_ref, inverse_ref, coarse_out, first_out):
    coarse = own_ref[...] + sub_ref[...] + grp_ref[...]
    coarse_out[...] = coarse
    first_out[...] = mm3(coarse, inverse_ref[...])


def first_step(own, sub, grp, inverse):
    shape = jax.ShapeDtypeStruct(own.shape, F32)
    return call(
        first_body,
        (shape, shape),
        "first",
        flops=own.size * 128 * 6,
        moved=own.size * 24,
        in_specs=[VMEM] * 4,
        out_specs=(VMEM,) * 2,
        limit=4 * 1024 * 1024,
    )(own, sub, grp, inverse)


def correct_body(index_ref, window_ref, coarse_ref, first_ref, matrix_ref, inverse_ref, local_ref, out_ref, product_ref):
    acc = None
    for k in range(matrix_ref.shape[0]):
        term = mm3(window_ref[index_ref[0, k]], matrix_ref[k])
        acc = term if acc is None else acc + term
    coarse = coarse_ref[...]
    result = first_ref[...] + mm3(coarse - acc, inverse_ref[...])
    out_ref[...] = result
    product_ref[...] = row_sums(coarse * result) + local_ref[...]


def correct(index, window, coarse, first, matrix, inverse, local):
    shape = jax.ShapeDtypeStruct(first.shape, F32)
    return call(
        correct_body,
        (shape, jax.ShapeDtypeStruct((8, first.shape[0]), F32)),
        "correct",
        flops=matrix.size * 128 * 6,
        moved=window.size * 4,
        in_specs=[SMEM] + [VMEM] * 6,
        out_specs=(VMEM, VMEM),
        limit=8 * 1024 * 1024,
    )(index, window, coarse, first, matrix, inverse, local)


def local_body(slots_ref, fresh_ref, factor_ref, aux_sub_ref, aux_grp_ref, out_ref, product_ref):
    width = factor_ref.shape[1]
    half = fresh_ref.shape[1] // 2
    per_face = half // width
    acc = jnp.zeros((fresh_ref.shape[0], width), F32)
    for which, aux in ((1, aux_sub_ref), (3, aux_grp_ref)):
        base = (which // 2) * half
        first = slots_ref[0, which] * per_face
        for b in range(per_face):
            cols = slice(base + b * width, base + (b + 1) * width)
            fresh = fresh_ref[:, cols]
            high, low = split(fresh * 0.5)
            mine = factor_ref[first + b]
            theirs = aux[b * width : (b + 1) * width, :].astype(BF16)
            pair = jnp.concatenate([mine, theirs], 1)
            middle = mm(jnp.concatenate([high, low], 1), twice(pair, 0))
            middle_high, middle_low = split(middle)
            solved = mm(middle_high, pair, NT) + mm(middle_low, pair, NT)
            solved = solved * 0.5
            out_ref[:, cols] = solved
            acc += fresh * solved
    product_ref[...] = row_sums(acc)


def local_solve(slots, fresh, factor, aux_sub, aux_grp):
    return call(
        local_body,
        (jax.ShapeDtypeStruct(fresh.shape, F32), jax.ShapeDtypeStruct((8, fresh.shape[0]), F32)),
        "local",
        flops=fresh.size * 128 * 16,
        moved=fresh.size * 12,
        in_specs=[SMEM] + [VMEM] * 4,
        out_specs=(VMEM, VMEM),
        limit=10 * 1024 * 1024,
    )(slots, fresh, factor, aux_sub, aux_grp)


def spread_body(slots_ref, solved_ref, own_ref, from_sub_ref, from_grp_ref, block_ref, basis_ref, aux_sub_ref, aux_grp_ref, out_ref):
    width = basis_ref.shape[1]
    prims = basis_ref.shape[0]
    half = solved_ref.shape[1] // 2
    per_face = half // width
    rows = half
    own = own_ref[...] * 0.5
    basis = basis_ref[...]
    for which, aux, other_ref in ((1, aux_sub_ref, from_sub_ref), (3, aux_grp_ref, from_grp_ref)):
        base = (which // 2) * half
        both = jnp.concatenate([own, other_ref[...] * 0.5], 1)
        right = jnp.concatenate([basis, aux[rows : rows + prims, :].astype(BF16)], 0)
        own_near = (block_ref[...] - slots_ref[0, which] * per_face).astype(F32)
        near = jnp.concatenate([own_near, aux[rows + prims : rows + prims + 1, :]], 1)
        for b in range(per_face):
            cols = slice(base + b * width, base + (b + 1) * width)
            high, low = split(jnp.where(near == b, both, 0.0))
            out_ref[:, cols] = solved_ref[:, cols] + (mm(high, right) + mm(low, right))


def spread(slots, solved, own, from_sub, from_grp, blocks, basis, aux_sub, aux_grp):
    return call(
        spread_body,
        jax.ShapeDtypeStruct(solved.shape, F32),
        "spread",
        flops=solved.size * 128 * 8,
        moved=solved.size * 12,
        in_specs=[SMEM] + [VMEM] * 8,
        out_specs=VMEM,
        limit=10 * 1024 * 1024,
    )(slots, solved, own, from_sub, from_grp, blocks, basis, aux_sub, aux_grp)


def shards(
    solution,
    residual,
    direction,
    residual_product,
    neighbor_slots,
    coupling,
    dirichlet_factor,
    face_block,
    neumann_factor,
    primal_block,
    primal_basis,
    coarse_matrix,
    coarse_block_inverse,
    coarse_pattern,
):
    width = face_block.shape[2]
    per_face = face_block.shape[1] // 4
    face_width = per_face * width
    own = direction[0]
    basis = primal_basis[0]
    factor = neumann_factor[0]
    product = residual_product[None, :]
    grp_count = lax.axis_size("grp")
    sub_count = lax.axis_size("sub")

    from_sub = shifted(own[:, :face_width], "sub", 1)
    from_grp = shifted(own[:, face_width:], "grp", 1)
    high, low = assemble(coupling[0], dirichlet_factor[0], face_block[0])
    aux_sub, aux_grp = pack(neighbor_slots, primal_block, basis, factor, per_face)
    aux_sub = shifted(aux_sub, "sub", -1)
    aux_grp = shifted(aux_grp, "grp", -1)

    y, curve = apply(neighbor_slots, own, from_sub, from_grp, high, low)
    back_sub = shifted(y[0], "sub", -1)
    back_grp = shifted(y[2], "grp", -1)
    curve = grand_total(curve)
    fresh, part, part_sub, part_grp = update(
        neighbor_slots, y, back_sub, back_grp, residual[0], curve, product, primal_block, basis, aux_sub, aux_grp
    )
    part_sub = shifted(part_sub, "sub", 1)
    part_grp = shifted(part_grp, "grp", 1)
    coarse, first = first_step(part, part_sub, part_grp, coarse_block_inverse[0])

    entry_sub = coarse_pattern // grp_count
    entry_grp = coarse_pattern % grp_count
    position = (entry_sub - lax.axis_index("sub") + REACH_SUBS) % sub_count
    index = position * grp_count + entry_grp
    column = lax.all_gather(first[None], "grp", axis=0, tiled=True)
    pieces = []
    for place in range(2 * REACH_SUBS + 1):
        pieces.append(column if place == REACH_SUBS else shifted(column, "sub", REACH_SUBS - place))
    window = jnp.concatenate(pieces, 0)

    solved, local = local_solve(neighbor_slots, fresh, factor, aux_sub, aux_grp)
    correction, partial = correct(
        index, window, coarse, first, coarse_matrix[0], coarse_block_inverse[0], local
    )
    other_sub = shifted(correction, "sub", -1)
    other_grp = shifted(correction, "grp", -1)
    new_product = grand_total(partial)[0]
    preconditioned = spread(
        neighbor_slots, solved, correction, other_sub, other_grp, primal_block, basis, aux_sub, aux_grp
    )
    step_length = residual_product / curve[0]
    new_solution = solution + step_length[None, :, None] * direction
    step_ratio = new_product / residual_product
    new_direction = preconditioned[None] + step_ratio[None, :, None] * direction
    return (new_solution, fresh[None], new_direction, new_product)


def solution(mesh):
    in_specs = (
        P(("sub", "grp"), None, None),
        P(("sub", "grp"), None, None),
        P(("sub", "grp"), None, None),
        P(),
        P(("sub", "grp"), None),
        P(("sub", "grp"), None, None, None),
        P(("sub", "grp"), None, None, None),
        P(("sub", "grp"), None, None, None),
        P(("sub", "grp"), None, None, None),
        P(("sub", "grp"), None),
        P(("sub", "grp"), None, None),
        P(("sub", "grp"), None, None, None),
        P(("sub", "grp"), None, None),
        P(("sub", "grp"), None),
    )
    out_specs = (
        P(("sub", "grp"), None, None),
        P(("sub", "grp"), None, None),
        P(("sub", "grp"), None, None),
        P(),
    )
    return jax.shard_map(shards, mesh=mesh, in_specs=in_specs, out_specs=out_specs, check_vma=False)
```

```python
import functools

import jax
import jax.numpy as jnp
from jax import lax
from jax.experimental import pallas as pl
from jax.experimental.pallas import tpu as pltpu
from jax.sharding import PartitionSpec as P

REACH_SUBS = 2
F32 = jnp.float32
BF16 = jnp.bfloat16
VMEM = pl.BlockSpec(memory_space=pltpu.VMEM)
SMEM = pl.BlockSpec(memory_space=pltpu.SMEM)
NN = (((1,), (0,)), ((), ()))
NT = (((1,), (1,)), ((), ()))


def shifted(value, axis, steps):
    count = lax.axis_size(axis)
    pairs = [(source, (source + steps) % count) for source in range(count)]
    return lax.ppermute(value, axis, pairs)


def total(value, axis):
    count = lax.axis_size(axis)
    if count & (count - 1):
        return lax.psum(value, axis)
    bit = 1
    while bit < count:
        value = value + lax.ppermute(value, axis, [(i, i ^ bit) for i in range(count)])
        bit *= 2
    return value


def grand_total(value):
    return total(total(value, "grp"), "sub")


def split(value):
    high = value.astype(BF16)
    low = (value - high.astype(F32)).astype(BF16)
    return high, low


def mm(a, b, dims=NN):
    return lax.dot_general(a, b, dims, preferred_element_type=F32)


def mm3(a, b):
    a_high, a_low = split(a)
    b_high, b_low = split(b)
    return mm(a_high, b_high) + (mm(a_low, b_high) + mm(a_high, b_low))


def twice(value, axis):
    return jnp.concatenate([value, value], axis=axis)


def row_sums(partial):
    ones = jnp.ones((8, partial.shape[1]), F32)
    return lax.dot_general(ones, partial, NT, precision=lax.Precision.HIGHEST, preferred_element_type=F32)


def per_row(row, width):
    tall = jnp.broadcast_to(row[0:1], (width, row.shape[1]))
    return tall.T


def call(body, out_shapes, name, flops, moved, scratch=(), grid=None, in_specs=None, out_specs=None, limit=None):
    params = {}
    if limit is not None:
        params["vmem_limit_bytes"] = limit
    kwargs = {}
    if grid is not None:
        kwargs["grid"] = grid
    return pl.pallas_call(
        body,
        out_shape=out_shapes,
        in_specs=in_specs,
        out_specs=out_specs,
        scratch_shapes=scratch,
        compiler_params=pltpu.CompilerParams(**params),
        cost_estimate=pl.CostEstimate(flops=flops, bytes_accessed=moved, transcendentals=0),
        name=name,
        **kwargs,
    )


BATCH = 8


def assemble_body(blocks, kept, couple_hbm, factor_hbm, face_hbm, *refs):
    sources = refs[:kept]
    high_ref, low_ref = refs[kept : kept + 2]
    targets = refs[kept + 2 : 2 * kept + 2]
    couple_ref, factor_ref, face_ref, inner_ref, middle_ref, near_ref, far_ref, sems, keep_sems = refs[2 * kept + 2 :]
    width = face_ref.shape[1]
    count = couple_ref.shape[0]
    reach = count // blocks
    pairs = blocks // 2
    rounds = count // BATCH

    def copy_of(i, which):
        part = pl.ds(i * BATCH, BATCH)
        source, target = ((factor_hbm, factor_ref), (couple_hbm, couple_ref))[which]
        return pltpu.make_async_copy(source.at[part], target.at[part], sems.at[which, i])

    def begin(i, carry):
        for which in range(2):
            copy_of(i, which).start()
        return carry

    face_copy = pltpu.make_async_copy(face_hbm, face_ref, keep_sems.at[kept])
    face_copy.start()
    lax.fori_loop(0, rounds, begin, 0)
    keeping = [pltpu.make_async_copy(a, b, keep_sems.at[i]) for i, (a, b) in enumerate(zip(sources, targets))]
    for copy in keeping:
        copy.start()
    face_copy.wait()

    def convert(block, carry):
        near_ref[block] = face_ref[block].astype(F32)
        far_ref[block] = jnp.zeros((width, width), F32)
        return carry

    lax.fori_loop(0, blocks, convert, 0)
    for extra in range(reach):
        far_ref[blocks + extra] = jnp.zeros((width, width), F32)

    def inner(i):
        for k in range(BATCH):
            factor = factor_ref[i * BATCH + k]
            high, low = split(mm(factor, factor, NT))
            inner_ref[i % 2, k, :width] = high
            inner_ref[i % 2, k, width:] = low

    def middle(i):
        for k in range(BATCH):
            high, low = split(mm(twice(couple_ref[i * BATCH + k], 1), inner_ref[i % 2, k]))
            middle_ref[i % 2, k, :, :width] = high
            middle_ref[i % 2, k, :, width:] = low

    def put(pair, row, half, value):
        high, low = split(value)
        cols = pl.ds(pl.multiple_of(half * width, width), width)
        high_ref[pair, row, :, cols] = high
        low_ref[pair, row, :, cols] = low

    def outer(i):
        per = blocks // BATCH
        q = i // per
        base = (i - q * per) * BATCH
        for k in range(BATCH):
            full = mm(middle_ref[i % 2, k], twice(couple_ref[i * BATCH + k], 1), NT)
            place = base + k
            reached = place + q + 1
            near_ref[place] += full[:width, :width]
            far_ref[reached] += full[width:, width:]
            wrapped = lax.rem(reached, blocks)
            half = lax.rem(wrapped, 2)
            put(wrapped // 2, reach - 1 - q + half, half, full[:width, width:])
            side = k % 2
            put(place // 2, reach + q + 1 + side, side, full[width:, :width])

    def wait(i, which):
        copy_of(i, which).wait()

    wait(0, 0)
    inner(0)
    wait(1, 0)
    wait(0, 1)
    inner(1)
    middle(0)

    def steady(i, carry):
        wait(i, 0)
        wait(i - 1, 1)
        inner(i)
        middle(i - 1)
        outer(i - 2)
        return carry

    lax.fori_loop(2, rounds, steady, 0)
    wait(rounds - 1, 1)
    middle(rounds - 1)
    outer(rounds - 2)
    outer(rounds - 1)

    def close(pair, carry):
        zero = jnp.zeros((width, width), BF16)
        for ref in (high_ref, low_ref):
            ref[pair, 2 * reach + 1, :, pl.ds(0, width)] = zero
            ref[pair, 0, :, pl.ds(width, width)] = zero
        for side in range(2):
            put(pair, reach + side, side, near_ref[2 * pair + side] + far_ref[2 * pair + side])
        return carry

    for extra in range(reach):
        far_ref[extra] += far_ref[blocks + extra]
    lax.fori_loop(0, pairs, close, 0)
    for copy in keeping:
        copy.wait()


def in_hbm(value):
    return pltpu.with_memory_space_constraint(value, pltpu.HBM)


def assemble(coupling, dirichlet, face, keep):
    blocks, width, _ = face.shape
    count = coupling.shape[0]
    reach = count // blocks
    pairs = blocks // 2
    shape = jax.ShapeDtypeStruct((pairs, 2 * reach + 2, width, 2 * width), BF16)
    hbm = pl.BlockSpec(memory_space=pltpu.HBM)
    return call(
        functools.partial(assemble_body, blocks, len(keep)),
        (shape, shape) + tuple(jax.ShapeDtypeStruct(k.shape, k.dtype) for k in keep),
        "assemble",
        flops=count * 2 * width**3 * 12,
        moved=coupling.size * 3,
        scratch=[
            pltpu.VMEM((count, 2 * width, width), BF16),
            pltpu.VMEM((count, width, width), BF16),
            pltpu.VMEM((blocks, width, width), BF16),
            pltpu.VMEM((2, BATCH, 2 * width, width), BF16),
            pltpu.VMEM((2, BATCH, 2 * width, 2 * width), BF16),
            pltpu.VMEM((blocks, width, width), F32),
            pltpu.VMEM((blocks + reach, width, width), F32),
            pltpu.SemaphoreType.DMA((2, count // BATCH)),
            pltpu.SemaphoreType.DMA((len(keep) + 1,)),
        ],
        in_specs=[hbm] * (3 + len(keep)),
        out_specs=(VMEM,) * (2 + len(keep)),
        limit=ASSEMBLE_LIMIT,
    )(in_hbm(coupling), in_hbm(dirichlet), in_hbm(face), *(in_hbm(k) for k in keep))


ASSEMBLE_LIMIT = 22 * 1024 * 1024


def apply_body(slots_ref, own_ref, from_sub_ref, from_grp_ref, high_ref, low_ref, out_ref, curve_ref, u_high, u_low):
    pairs, count, width, _ = high_ref.shape
    reach = count // 2 - 1
    face_width = from_sub_ref.shape[1]
    per_face = face_width // width
    blocks = 2 * pairs
    loads = own_ref.shape[0]
    faces = ((from_sub_ref, 0), (own_ref, 0), (from_grp_ref, 0), (own_ref, face_width))
    for which, (ref, base) in enumerate(faces):
        slot = slots_ref[0, which]
        for b in range(per_face):
            high, low = split(ref[:, base + b * width : base + (b + 1) * width])
            place = slot * per_face + b + reach
            u_high[place] = high
            u_low[place] = low
    for ref in (u_high, u_low):
        for i in range(reach):
            ref[i] = ref[blocks + i]
        for i in range(reach + 1):
            ref[blocks + reach + i] = ref[reach + i]
    half_face = per_face // 2

    def one_face(which, carry):
        slot = slots_ref[0, which]
        for part in range(half_face):
            pair = slot * half_face + part
            high = jnp.concatenate([u_high[2 * pair + i] for i in range(count)], 1)
            low = jnp.concatenate([u_low[2 * pair + i] for i in range(count)], 1)
            weight = high_ref[pair].reshape(count * width, 2 * width)
            both = mm(jnp.concatenate([high, low], 0), weight)
            result = both[:loads] + both[loads:] + mm(high, low_ref[pair].reshape(count * width, 2 * width))
            out_ref[which, :, part * 2 * width : (part + 1) * 2 * width] = result
        return carry

    lax.fori_loop(0, 4, one_face, 0)
    acc = jnp.zeros((loads, width), F32)
    for which, (ref, base) in enumerate(faces):
        for b in range(per_face):
            acc += ref[:, base + b * width : base + (b + 1) * width] * out_ref[which, :, b * width : (b + 1) * width]
    curve_ref[...] = row_sums(acc)


def apply(slots, own, from_sub, from_grp, high, low):
    pairs, count, width, double = high.shape
    loads, face_width = from_sub.shape
    return call(
        apply_body,
        (
            jax.ShapeDtypeStruct((4, loads, face_width), F32),
            jax.ShapeDtypeStruct((8, loads), F32),
        ),
        "apply",
        flops=high.size * loads * 6,
        moved=high.size * 4,
        scratch=[pltpu.VMEM((2 * pairs + count - 1, loads, width), BF16)] * 2,
        in_specs=[SMEM] + [VMEM] * 5,
        out_specs=(VMEM, VMEM),
        limit=6 * 1024 * 1024,
    )(slots, own, from_sub, from_grp, high, low)


def pack_body(per_face, slots_ref, block_hbm, basis_hbm, factor_hbm, sub_ref, grp_ref, block_ref, basis_ref, factor_ref, sems):
    prims, width = basis_ref.shape
    rows = per_face * width
    copies = [
        pltpu.make_async_copy(basis_hbm, basis_ref, sems.at[2]),
        pltpu.make_async_copy(block_hbm, block_ref, sems.at[3]),
    ]
    for i, which in enumerate((0, 2)):
        part = pl.ds(slots_ref[0, which] * per_face, per_face)
        copies.append(pltpu.make_async_copy(factor_hbm.at[part], factor_ref.at[i], sems.at[i]))
    for copy in copies:
        copy.start()
    for copy in copies:
        copy.wait()
    for i, (out, which) in enumerate(((sub_ref, 0), (grp_ref, 2))):
        first = slots_ref[0, which] * per_face
        for b in range(per_face):
            out[b * width : (b + 1) * width, :] = factor_ref[i, b].astype(F32)
        out[rows : rows + prims, :] = basis_ref[...].astype(F32)
        near = (block_ref[...] - first).astype(F32)
        out[rows + prims :, :] = jnp.broadcast_to(near, (8, width))


def pack(slots, blocks, basis, factor, per_face):
    prims, width = basis.shape
    shape = jax.ShapeDtypeStruct((per_face * width + prims + 8, width), F32)
    hbm = pl.BlockSpec(memory_space=pltpu.HBM)
    return call(
        functools.partial(pack_body, per_face),
        (shape, shape),
        "pack",
        flops=1000,
        moved=shape.size * 12,
        scratch=[
            pltpu.VMEM(blocks.shape, jnp.int32),
            pltpu.VMEM((prims, width), BF16),
            pltpu.VMEM((2, per_face, width, width), BF16),
            pltpu.SemaphoreType.DMA((4,)),
        ],
        in_specs=[SMEM, hbm, hbm, hbm],
        out_specs=(VMEM, VMEM),
        limit=4 * 1024 * 1024,
    )(slots, in_hbm(blocks), in_hbm(basis), in_hbm(factor))


def update_body(slots_ref, y_ref, back_sub_ref, back_grp_ref, residual_ref, curve_ref, product_ref, block_ref, basis_ref, aux_sub_ref, aux_grp_ref, residual_out, half_out, own_out, sub_out, grp_out):
    width = basis_ref.shape[1]
    prims = basis_ref.shape[0]
    face_width = back_sub_ref.shape[1]
    per_face = face_width // width
    rows = face_width
    scale = per_row(product_ref[...] / curve_ref[...], width)
    basis = basis_ref[...].astype(F32).T
    own_total = None
    for which, back, aux, out in (
        (1, back_sub_ref, aux_sub_ref, sub_out),
        (3, back_grp_ref, aux_grp_ref, grp_out),
    ):
        offset = (which // 2) * face_width
        other = aux[rows : rows + prims, :].T
        own_near = block_ref[...] - slots_ref[0, which] * per_face
        other_near = aux[rows + prims : rows + prims + 1, :]
        lefts = []
        rights = []
        for b in range(per_face):
            cols = slice(b * width, (b + 1) * width)
            image = y_ref[which, :, cols] + back[:, cols]
            fresh = residual_ref[:, offset + b * width : offset + (b + 1) * width] - scale * image
            residual_out[:, offset + b * width : offset + (b + 1) * width] = fresh
            half = fresh * 0.5
            half_out[:, offset + b * width : offset + (b + 1) * width] = half
            lefts.append(half)
            mine = jnp.where(own_near == b, basis, 0.0).astype(BF16)
            theirs = jnp.where(other_near == b, other, 0.0).astype(BF16)
            rights.append(jnp.concatenate([mine, theirs], 1))
        high, low = split(jnp.concatenate(lefts, 1))
        right = jnp.concatenate(rights, 0)
        both = mm(high, right) + mm(low, right)
        own = both[:, :prims]
        own_total = own if own_total is None else own_total + own
        out[...] = both[:, prims:]
    own_out[...] = own_total


def update(slots, y, back_sub, back_grp, residual, curve, product, blocks, basis, aux_sub, aux_grp):
    loads = residual.shape[0]
    prims = basis.shape[0]
    small = jax.ShapeDtypeStruct((loads, prims), F32)
    return call(
        update_body,
        (jax.ShapeDtypeStruct(residual.shape, F32), jax.ShapeDtypeStruct(residual.shape, F32), small, small, small),
        "update",
        flops=residual.size * prims * 8,
        moved=residual.size * 20,
        in_specs=[SMEM] + [VMEM] * 10,
        out_specs=(VMEM,) * 5,
        limit=16 * 1024 * 1024,
    )(slots, y, back_sub, back_grp, residual, curve, product, blocks, basis, aux_sub, aux_grp)


def first_body(own_ref, sub_ref, grp_ref, inverse_ref, local_ref, coarse_out, first_out, local_out):
    coarse = own_ref[...] + sub_ref[...] + grp_ref[...]
    coarse_out[...] = coarse
    first_out[...] = mm3(coarse, inverse_ref[...])
    local_out[...] = local_ref[...]


def first_step(own, sub, grp, inverse, local):
    shape = jax.ShapeDtypeStruct(own.shape, F32)
    return call(
        first_body,
        (shape, shape, jax.ShapeDtypeStruct(local.shape, F32)),
        "first",
        flops=own.size * 128 * 6,
        moved=own.size * 24,
        in_specs=[VMEM] * 5,
        out_specs=(VMEM,) * 3,
        limit=4 * 1024 * 1024,
    )(own, sub, grp, inverse, local)


def merge_body(*refs):
    out_ref = refs[-1]
    for place, ref in enumerate(refs[:-1]):
        size = ref.shape[0]
        out_ref[place * size : (place + 1) * size] = ref[...]


def merge(pieces):
    size = pieces[0].shape[0]
    shape = jax.ShapeDtypeStruct((size * len(pieces),) + pieces[0].shape[1:], F32)
    return call(
        merge_body,
        shape,
        "merge",
        flops=1000,
        moved=shape.size * 8,
        in_specs=[VMEM] * len(pieces),
        out_specs=VMEM,
        limit=4 * 1024 * 1024,
    )(*pieces)


def correct_body(paired, pattern_ref, window_ref, beside_ref, coarse_ref, first_ref, matrix_ref, inverse_ref, local_ref, out_ref, product_ref, held_ref):
    size = window_ref.shape[0]
    held_ref[:size] = window_ref[...]
    held_ref[size:] = beside_ref[...]
    grp_count = lax.axis_size("grp")
    sub_count = lax.axis_size("sub")
    my_sub = lax.axis_index("sub")
    my_grp = lax.axis_index("grp")
    acc = None
    for k in range(matrix_ref.shape[0]):
        entry = pattern_ref[0, k]
        entry_sub = entry // grp_count
        entry_grp = entry - entry_sub * grp_count
        position = lax.rem(entry_sub - my_sub + REACH_SUBS + sub_count, sub_count)
        if paired:
            apart = entry_grp ^ my_grp
            index = ((apart & 1) * (2 * REACH_SUBS + 1) + position) * 2 + (apart >> 1)
        else:
            index = position * grp_count + entry_grp
        term = mm3(held_ref[index], matrix_ref[k])
        acc = term if acc is None else acc + term
    coarse = coarse_ref[...]
    result = first_ref[...] + mm3(coarse - acc, inverse_ref[...])
    out_ref[...] = result
    product_ref[...] = row_sums(coarse * result) + local_ref[...]


def correct(paired, pattern, window, beside, coarse, first, matrix, inverse, local):
    shape = jax.ShapeDtypeStruct(first.shape, F32)
    return call(
        functools.partial(correct_body, paired),
        (shape, jax.ShapeDtypeStruct((8, first.shape[0]), F32)),
        "correct",
        flops=matrix.size * 128 * 6,
        moved=window.size * 4,
        scratch=[pltpu.VMEM((window.shape[0] + beside.shape[0],) + window.shape[1:], F32)],
        in_specs=[SMEM] + [VMEM] * 7,
        out_specs=(VMEM, VMEM),
        limit=8 * 1024 * 1024,
    )(pattern, window, beside, coarse, first, matrix, inverse, local)


def local_body(slots_ref, halved_ref, factor_ref, aux_sub_ref, aux_grp_ref, out_ref, product_ref):
    width = factor_ref.shape[1]
    half = halved_ref.shape[1] // 2
    per_face = half // width
    acc = jnp.zeros((halved_ref.shape[0], width), F32)
    for which, aux in ((1, aux_sub_ref), (3, aux_grp_ref)):
        base = (which // 2) * half
        first = slots_ref[0, which] * per_face
        for b in range(per_face):
            cols = slice(base + b * width, base + (b + 1) * width)
            halved = halved_ref[:, cols]
            high, low = split(halved)
            mine = factor_ref[first + b]
            theirs = aux[b * width : (b + 1) * width, :].astype(BF16)
            pair = jnp.concatenate([mine, theirs], 1)
            middle = mm(jnp.concatenate([high, low], 1), twice(pair, 0))
            middle_high, middle_low = split(middle)
            solved = mm(middle_high, pair, NT) + mm(middle_low, pair, NT)
            out_ref[:, cols] = solved * 0.5
            acc += halved * solved
    product_ref[...] = row_sums(acc)


def local_solve(slots, fresh, factor, aux_sub, aux_grp):
    return call(
        local_body,
        (jax.ShapeDtypeStruct(fresh.shape, F32), jax.ShapeDtypeStruct((8, fresh.shape[0]), F32)),
        "local",
        flops=fresh.size * 128 * 16,
        moved=fresh.size * 12,
        in_specs=[SMEM] + [VMEM] * 4,
        out_specs=(VMEM, VMEM),
        limit=10 * 1024 * 1024,
    )(slots, fresh, factor, aux_sub, aux_grp)


def spread_body(slots_ref, solved_ref, own_ref, from_sub_ref, from_grp_ref, block_ref, basis_ref, aux_sub_ref, aux_grp_ref, iterate_ref, direction_ref, curve_ref, product_ref, out_ref, iterate_out):
    width = basis_ref.shape[1]
    prims = basis_ref.shape[0]
    half = solved_ref.shape[1] // 2
    per_face = half // width
    rows = half
    own = own_ref[...] * 0.5
    basis = basis_ref[...]
    scale = per_row(product_ref[...] / curve_ref[...], width)
    for which, aux, other_ref in ((1, aux_sub_ref, from_sub_ref), (3, aux_grp_ref, from_grp_ref)):
        base = (which // 2) * half
        both = jnp.concatenate([own, other_ref[...] * 0.5], 1)
        right = jnp.concatenate([basis, aux[rows : rows + prims, :].astype(BF16)], 0)
        own_near = (block_ref[...] - slots_ref[0, which] * per_face).astype(F32)
        near = jnp.concatenate([own_near, aux[rows + prims : rows + prims + 1, :]], 1)
        for b in range(per_face):
            cols = slice(base + b * width, base + (b + 1) * width)
            high, low = split(jnp.where(near == b, both, 0.0))
            out_ref[:, cols] = solved_ref[:, cols] + (mm(high, right) + mm(low, right))
            iterate_out[:, cols] = iterate_ref[:, cols] + scale * direction_ref[:, cols]


def spread(slots, solved, own, from_sub, from_grp, blocks, basis, aux_sub, aux_grp, iterate, direction, curve, product):
    return call(
        spread_body,
        (jax.ShapeDtypeStruct(solved.shape, F32),) * 2,
        "spread",
        flops=solved.size * 128 * 8,
        moved=solved.size * 12,
        in_specs=[SMEM] + [VMEM] * 12,
        out_specs=(VMEM, VMEM),
        limit=10 * 1024 * 1024,
    )(slots, solved, own, from_sub, from_grp, blocks, basis, aux_sub, aux_grp, iterate, direction, curve, product)


def shards(
    solution,
    residual,
    direction,
    residual_product,
    neighbor_slots,
    coupling,
    dirichlet_factor,
    face_block,
    neumann_factor,
    primal_block,
    primal_basis,
    coarse_matrix,
    coarse_block_inverse,
    coarse_pattern,
):
    width = face_block.shape[2]
    per_face = face_block.shape[1] // 4
    face_width = per_face * width
    own = direction[0]
    basis = primal_basis[0]
    factor = neumann_factor[0]
    product = residual_product[None, :]
    grp_count = lax.axis_size("grp")

    from_sub = shifted(own[:, :face_width], "sub", 1)
    from_grp = shifted(own[:, face_width:], "grp", 1)
    aux_sub, aux_grp = pack(neighbor_slots, primal_block, basis, factor, per_face)
    aux_sub = shifted(aux_sub, "sub", -1)
    aux_grp = shifted(aux_grp, "grp", -1)
    keep = (own, residual[0], factor, basis, coarse_matrix[0], coarse_block_inverse[0], primal_block, solution[0])
    high, low, own, old, factor, basis, matrix, inverse, blocks, iterate = assemble(
        coupling[0], dirichlet_factor[0], face_block[0], keep
    )

    y, curve = apply(neighbor_slots, own, from_sub, from_grp, high, low)
    back_sub = shifted(y[0], "sub", -1)
    back_grp = shifted(y[2], "grp", -1)
    curve = grand_total(curve)
    fresh, halved, part, part_sub, part_grp = update(
        neighbor_slots, y, back_sub, back_grp, old, curve, product, blocks, basis, aux_sub, aux_grp
    )
    part_sub = shifted(part_sub, "sub", 1)
    part_grp = shifted(part_grp, "grp", 1)
    solved, local = local_solve(neighbor_slots, halved, factor, aux_sub, aux_grp)
    coarse, first, local = first_step(part, part_sub, part_grp, inverse, local)

    if grp_count == 4:
        group = jnp.stack([first, shifted(first, "grp", 2)], 0)
    else:
        group = lax.all_gather(first[None], "grp", axis=0, tiled=True)
    pieces = []
    for place in range(2 * REACH_SUBS + 1):
        pieces.append(group if place == REACH_SUBS else shifted(group, "sub", REACH_SUBS - place))
    window = merge(pieces)
    beside = window[:1]
    if grp_count == 4:
        beside = lax.ppermute(window, "grp", [(i, i ^ 1) for i in range(grp_count)])

    correction, partial = correct(grp_count == 4, coarse_pattern, window, beside, coarse, first, matrix, inverse, local)
    other_sub = shifted(correction, "sub", -1)
    other_grp = shifted(correction, "grp", -1)
    partial = total(partial, "grp")
    partial, other_sub, other_grp = lax.optimization_barrier((partial, other_sub, other_grp))
    preconditioned, new_solution = spread(
        neighbor_slots, solved, correction, other_sub, other_grp, blocks, basis, aux_sub, aux_grp, iterate, own, curve, product
    )
    new_product = total(partial, "sub")[0]
    step_ratio = new_product / residual_product
    new_direction = preconditioned[None] + step_ratio[None, :, None] * own[None]
    return (new_solution[None], fresh[None], new_direction, new_product)


def solution(mesh):
    in_specs = (
        P(("sub", "grp"), None, None),
        P(("sub", "grp"), None, None),
        P(("sub", "grp"), None, None),
        P(),
        P(("sub", "grp"), None),
        P(("sub", "grp"), None, None, None),
        P(("sub", "grp"), None, None, None),
        P(("sub", "grp"), None, None, None),
        P(("sub", "grp"), None, None, None),
        P(("sub", "grp"), None),
        P(("sub", "grp"), None, None),
        P(("sub", "grp"), None, None, None),
        P(("sub", "grp"), None, None),
        P(("sub", "grp"), None),
    )
    out_specs = (
        P(("sub", "grp"), None, None),
        P(("sub", "grp"), None, None),
        P(("sub", "grp"), None, None),
        P(),
    )
    return jax.shard_map(shards, mesh=mesh, in_specs=in_specs, out_specs=out_specs, check_vma=False)
```

```python
import functools

import jax
import jax.numpy as jnp
from jax import lax
from jax.experimental import pallas as pl
from jax.experimental.pallas import tpu as pltpu
from jax.sharding import PartitionSpec as P


REACH_SUBS = 2
F32 = jnp.float32
BF16 = jnp.bfloat16
VMEM = pl.BlockSpec(memory_space=pltpu.VMEM)
SMEM = pl.BlockSpec(memory_space=pltpu.SMEM)
NN = (((1,), (0,)), ((), ()))
NT = (((1,), (1,)), ((), ()))


def shifted(value, axis, steps):
    count = lax.axis_size(axis)
    pairs = [(source, (source + steps) % count) for source in range(count)]
    return lax.ppermute(value, axis, pairs)


def total(value, axis):
    count = lax.axis_size(axis)
    if count & (count - 1):
        return lax.psum(value, axis)
    bits = [1 << k for k in range(count.bit_length() - 1)]
    for bit in reversed(bits) if axis == "sub" else bits:
        value = value + lax.ppermute(value, axis, [(i, i ^ bit) for i in range(count)])
    return value


def total_with(value, axis, late):
    count = lax.axis_size(axis)
    if count & (count - 1):
        value, extra = late(value)
        return lax.psum(value, axis), extra
    bit = 1
    extra = None
    while bit < count:
        if 2 * bit == count:
            value, extra = late(value)
        value = value + lax.ppermute(value, axis, [(i, i ^ bit) for i in range(count)])
        bit *= 2
    return value, extra


def swapped_window(count):
    return REACH_SUBS == 2 and count % 4 == 0 and count > 4


def sub_window(group):
    count = lax.axis_size("sub")
    everyone = range(count)
    if swapped_window(count):
        targets = (
            [i ^ 1 for i in everyone],
            [(i - 1 + 2 * (i & 1)) % count for i in everyone],
            [i ^ 2 for i in everyone],
            [(i - 2 + 2 * (i & 2)) % count for i in everyone],
        )
    else:
        targets = [[(i - step) % count for i in everyone] for step in range(-REACH_SUBS, REACH_SUBS + 1) if step]
    pieces = []
    for target in targets:
        pieces.append(lax.ppermute(group, "sub", list(zip(everyone, target))))
    return pieces


def sub_slot(offset, mine, count):
    if swapped_window(count):
        far = jnp.where((mine & 2 == 0) == (offset == 2), 3, 4)
        near = jnp.where((mine & 1 == 0) == (offset == 1), 1, 2)
        return jnp.where(offset == 0, 0, jnp.where((offset == 1) | (offset == -1), near, far))
    return jnp.where(offset == 0, 0, offset + REACH_SUBS + (offset < 0).astype(jnp.int32))


def split(value):
    high = value.astype(BF16)
    low = (value - high.astype(F32)).astype(BF16)
    return high, low


def mm(a, b, dims=NN):
    return lax.dot_general(a, b, dims, preferred_element_type=F32)


def mm3(a, b):
    a_high, a_low = split(a)
    b_high, b_low = split(b)
    return mm(a_high, b_high) + (mm(a_low, b_high) + mm(a_high, b_low))


def twice(value, axis):
    return jnp.concatenate([value, value], axis=axis)


def row_sums(partial):
    ones = jnp.ones((8, partial.shape[1]), F32)
    return lax.dot_general(ones, partial, NT, precision=lax.Precision.HIGHEST, preferred_element_type=F32)


def per_row(row, width):
    tall = jnp.broadcast_to(row[0:1], (width, row.shape[1]))
    return tall.T


def call(body, out_shapes, flops, moved, scratch=(), grid=None, in_specs=None, out_specs=None, limit=None):
    params = {}
    if limit is not None:
        params["vmem_limit_bytes"] = limit
    kwargs = {}
    if grid is not None:
        kwargs["grid"] = grid
    return pl.pallas_call(
        body,
        out_shape=out_shapes,
        in_specs=in_specs,
        out_specs=out_specs,
        scratch_shapes=scratch,
        compiler_params=pltpu.CompilerParams(**params),
        cost_estimate=pl.CostEstimate(flops=flops, bytes_accessed=moved, transcendentals=0),
        **kwargs,
    )


BATCH = 16


def in_hbm(value):
    return pltpu.with_memory_space_constraint(value, pltpu.HBM)


def prepare_body(kept, couple_hbm, factor_hbm, *refs):
    sources = refs[:kept]
    couple_ref, middle_ref = refs[kept : kept + 2]
    targets = refs[kept + 2 : 2 * kept + 2]
    factor_ref, inner_ref, sems, keep_sems = refs[2 * kept + 2 :]
    width = factor_ref.shape[1]
    rounds = couple_ref.shape[0] // BATCH

    def copy_of(i, which):
        part = pl.ds(i * BATCH, BATCH)
        source, target = ((factor_hbm, factor_ref), (couple_hbm, couple_ref))[which]
        return pltpu.make_async_copy(source.at[part], target.at[part], sems.at[which, i])

    def begin(i, carry):
        for which in range(2):
            copy_of(i, which).start()
        return carry

    keeping = [pltpu.make_async_copy(a, b, keep_sems.at[i]) for i, (a, b) in enumerate(zip(sources, targets))]
    lax.fori_loop(0, rounds, begin, 0)
    for copy in keeping:
        copy.start()

    def inner(i):
        for k in range(BATCH):
            factor = factor_ref[i * BATCH + k]
            high, low = split(mm(factor, factor, NT))
            inner_ref[i % 2, k, :width] = high
            inner_ref[i % 2, k, width:] = low

    def middle(i):
        for k in range(BATCH):
            high, low = split(mm(twice(couple_ref[i * BATCH + k], 1), inner_ref[i % 2, k]))
            middle_ref[i * BATCH + k, :, :width] = high
            middle_ref[i * BATCH + k, :, width:] = low

    copy_of(0, 0).wait()
    inner(0)

    def steady(i, carry):
        copy_of(i, 0).wait()
        copy_of(i - 1, 1).wait()
        inner(i)
        middle(i - 1)
        return carry

    lax.fori_loop(1, rounds, steady, 0)
    copy_of(rounds - 1, 1).wait()
    middle(rounds - 1)
    for copy in keeping:
        copy.wait()


def prepare(coupling, dirichlet, keep):
    count, double, width = coupling.shape
    hbm = pl.BlockSpec(memory_space=pltpu.HBM)
    return call(
        functools.partial(prepare_body, len(keep)),
        (
            jax.ShapeDtypeStruct(coupling.shape, BF16),
            jax.ShapeDtypeStruct((count, double, double), BF16),
        )
        + tuple(jax.ShapeDtypeStruct(k.shape, k.dtype) for k in keep),
        flops=count * 2 * width**3 * 6,
        moved=coupling.size * 3,
        scratch=[
            pltpu.VMEM((count, width, width), BF16),
            pltpu.VMEM((2, BATCH, double, width), BF16),
            pltpu.SemaphoreType.DMA((2, count // BATCH)),
            pltpu.SemaphoreType.DMA((len(keep),)),
        ],
        in_specs=[hbm] * (2 + len(keep)),
        out_specs=(VMEM,) * (2 + len(keep)),
        limit=6 * 1024 * 1024,
    )(in_hbm(coupling), in_hbm(dirichlet), *(in_hbm(k) for k in keep))


def assemble_body(blocks, kept, couple_ref, middle_ref, face_ref, *refs):
    sources = refs[:kept]
    high_ref, low_ref = refs[kept : kept + 2]
    targets = refs[kept + 2 : 2 * kept + 2]
    near_ref, far_ref, keep_sems = refs[2 * kept + 2 :]
    width = face_ref.shape[1]
    count = couple_ref.shape[0]
    reach = count // blocks
    pairs = blocks // 2
    keeping = [pltpu.make_async_copy(a, b, keep_sems.at[i]) for i, (a, b) in enumerate(zip(sources, targets))]
    for copy in keeping:
        copy.start()

    def convert(block, carry):
        near_ref[block] = face_ref[block].astype(F32)
        far_ref[block] = jnp.zeros((width, width), F32)
        return carry

    lax.fori_loop(0, blocks, convert, 0)
    for extra in range(reach):
        far_ref[blocks + extra] = jnp.zeros((width, width), F32)

    def put(pair, row, half, value):
        high, low = split(value)
        cols = pl.ds(pl.multiple_of(half * width, width), width)
        high_ref[pair, row, :, cols] = high
        low_ref[pair, row, :, cols] = low

    def outer(i, carry):
        per = blocks // BATCH
        q = i // per
        base = (i - q * per) * BATCH
        for k in range(BATCH):
            full = mm(middle_ref[i * BATCH + k], twice(couple_ref[i * BATCH + k], 1), NT)
            place = base + k
            reached = place + q + 1
            near_ref[place] += full[:width, :width]
            far_ref[reached] += full[width:, width:]
            wrapped = lax.rem(reached, blocks)
            half = lax.rem(wrapped, 2)
            put(wrapped // 2, reach - 1 - q + half, half, full[:width, width:])
            side = k % 2
            put(place // 2, reach + q + 1 + side, side, full[width:, :width])
        return carry

    lax.fori_loop(0, count // BATCH, outer, 0)

    def close(pair, carry):
        zero = jnp.zeros((width, width), BF16)
        for ref in (high_ref, low_ref):
            ref[pair, 2 * reach + 1, :, pl.ds(0, width)] = zero
            ref[pair, 0, :, pl.ds(width, width)] = zero
        for side in range(2):
            put(pair, reach + side, side, near_ref[2 * pair + side] + far_ref[2 * pair + side])
        return carry

    for extra in range(reach):
        far_ref[extra] += far_ref[blocks + extra]
    lax.fori_loop(0, pairs, close, 0)
    for copy in keeping:
        copy.wait()


def assemble(couple, middle, face, keep):
    blocks, width, _ = face.shape
    count = couple.shape[0]
    reach = count // blocks
    pairs = blocks // 2
    shape = jax.ShapeDtypeStruct((pairs, 2 * reach + 2, width, 2 * width), BF16)
    hbm = pl.BlockSpec(memory_space=pltpu.HBM)
    return call(
        functools.partial(assemble_body, blocks, len(keep)),
        (shape, shape) + tuple(jax.ShapeDtypeStruct(k.shape, k.dtype) for k in keep),
        flops=count * 2 * width**3 * 6,
        moved=couple.size * 3,
        scratch=[
            pltpu.VMEM((blocks, width, width), F32),
            pltpu.VMEM((blocks + reach, width, width), F32),
            pltpu.SemaphoreType.DMA((len(keep),)),
        ],
        in_specs=[VMEM] * 3 + [hbm] * len(keep),
        out_specs=(VMEM,) * (2 + len(keep)),
        limit=6 * 1024 * 1024,
    )(couple, middle, face, *(in_hbm(k) for k in keep))


def apply_body(slots_ref, own_ref, from_sub_ref, from_grp_ref, high_ref, low_ref, out_ref, curve_ref, u_high, u_low):
    pairs, count, width, _ = high_ref.shape
    reach = count // 2 - 1
    face_width = from_sub_ref.shape[1]
    per_face = face_width // width
    blocks = 2 * pairs
    loads = own_ref.shape[0]
    faces = ((from_sub_ref, 0), (own_ref, 0), (from_grp_ref, 0), (own_ref, face_width))
    for which, (ref, base) in enumerate(faces):
        slot = slots_ref[0, which]
        for b in range(per_face):
            high, low = split(ref[:, base + b * width : base + (b + 1) * width])
            place = slot * per_face + b + reach
            u_high[place] = high
            u_low[place] = low
    for ref in (u_high, u_low):
        for i in range(reach):
            ref[i] = ref[blocks + i]
        for i in range(reach + 1):
            ref[blocks + reach + i] = ref[reach + i]
    half_face = per_face // 2

    def one_face(which, carry):
        slot = slots_ref[0, which]
        for part in range(half_face):
            pair = slot * half_face + part
            high = jnp.concatenate([u_high[2 * pair + i] for i in range(count)], 1)
            low = jnp.concatenate([u_low[2 * pair + i] for i in range(count)], 1)
            weight = high_ref[pair].reshape(count * width, 2 * width)
            both = mm(jnp.concatenate([high, low], 0), weight)
            result = both[:loads] + both[loads:] + mm(high, low_ref[pair].reshape(count * width, 2 * width))
            out_ref[which, :, part * 2 * width : (part + 1) * 2 * width] = result
        return carry

    lax.fori_loop(0, 4, one_face, 0)
    acc = jnp.zeros((loads, width), F32)
    for which, (ref, base) in enumerate(faces):
        for b in range(per_face):
            acc += ref[:, base + b * width : base + (b + 1) * width] * out_ref[which, :, b * width : (b + 1) * width]
    curve_ref[...] = row_sums(acc)


def apply(slots, own, from_sub, from_grp, high, low):
    pairs, count, width, _ = high.shape
    loads, face_width = from_sub.shape
    return call(
        apply_body,
        (
            jax.ShapeDtypeStruct((4, loads, face_width), F32),
            jax.ShapeDtypeStruct((8, loads), F32),
        ),
        flops=high.size * loads * 6,
        moved=high.size * 4,
        scratch=[pltpu.VMEM((2 * pairs + count - 1, loads, width), BF16)] * 2,
        in_specs=[SMEM] + [VMEM] * 5,
        out_specs=(VMEM, VMEM),
        limit=6 * 1024 * 1024,
    )(slots, own, from_sub, from_grp, high, low)


def pack_body(per_face, slots_ref, block_ref, basis_ref, factor_ref, sub_ref, grp_ref):
    prims, width = basis_ref.shape
    rows = per_face * width
    for out, which in ((sub_ref, 0), (grp_ref, 2)):
        first = slots_ref[0, which] * per_face
        for b in range(per_face):
            out[b * width : (b + 1) * width, :] = factor_ref[first + b].astype(F32)
        out[rows : rows + prims, :] = basis_ref[...].astype(F32)
        near = (block_ref[...] - first).astype(F32)
        out[rows + prims :, :] = jnp.broadcast_to(near, (8, width))


def pack(slots, blocks, basis, factor, per_face):
    prims, width = basis.shape
    shape = jax.ShapeDtypeStruct((per_face * width + prims + 8, width), F32)
    return call(
        functools.partial(pack_body, per_face),
        (shape, shape),
        flops=1000,
        moved=shape.size * 12,
        in_specs=[SMEM] + [VMEM] * 3,
        out_specs=(VMEM, VMEM),
        limit=4 * 1024 * 1024,
    )(slots, blocks, basis, factor)


def update_body(slots_ref, y_ref, back_sub_ref, back_grp_ref, residual_ref, curve_ref, product_ref, block_ref, basis_ref, aux_sub_ref, aux_grp_ref, residual_out, half_out, own_out, sub_out, grp_out):
    width = basis_ref.shape[1]
    prims = basis_ref.shape[0]
    face_width = back_sub_ref.shape[1]
    per_face = face_width // width
    rows = face_width
    scale = per_row(product_ref[...] / curve_ref[...], width)
    basis = basis_ref[...].astype(F32).T
    own_total = None
    for which, back, aux, out in (
        (1, back_sub_ref, aux_sub_ref, sub_out),
        (3, back_grp_ref, aux_grp_ref, grp_out),
    ):
        offset = (which // 2) * face_width
        other = aux[rows : rows + prims, :].T
        own_near = block_ref[...] - slots_ref[0, which] * per_face
        other_near = aux[rows + prims : rows + prims + 1, :]
        lefts = []
        rights = []
        for b in range(per_face):
            cols = slice(b * width, (b + 1) * width)
            image = y_ref[which, :, cols] + back[:, cols]
            fresh = residual_ref[:, offset + b * width : offset + (b + 1) * width] - scale * image
            residual_out[:, offset + b * width : offset + (b + 1) * width] = fresh
            half = fresh * 0.5
            half_out[:, offset + b * width : offset + (b + 1) * width] = half
            lefts.append(half)
            mine = jnp.where(own_near == b, basis, 0.0).astype(BF16)
            theirs = jnp.where(other_near == b, other, 0.0).astype(BF16)
            rights.append(jnp.concatenate([mine, theirs], 1))
        high, low = split(jnp.concatenate(lefts, 1))
        right = jnp.concatenate(rights, 0)
        both = mm(high, right) + mm(low, right)
        own = both[:, :prims]
        own_total = own if own_total is None else own_total + own
        out[...] = both[:, prims:]
    own_out[...] = own_total


def update(slots, y, back_sub, back_grp, residual, curve, product, blocks, basis, aux_sub, aux_grp):
    loads = residual.shape[0]
    prims = basis.shape[0]
    small = jax.ShapeDtypeStruct((loads, prims), F32)
    return call(
        update_body,
        (jax.ShapeDtypeStruct(residual.shape, F32), jax.ShapeDtypeStruct(residual.shape, F32), small, small, small),
        flops=residual.size * prims * 8,
        moved=residual.size * 20,
        in_specs=[SMEM] + [VMEM] * 10,
        out_specs=(VMEM,) * 5,
        limit=16 * 1024 * 1024,
    )(slots, y, back_sub, back_grp, residual, curve, product, blocks, basis, aux_sub, aux_grp)


def first_body(own_ref, sub_ref, grp_ref, inverse_ref, coarse_out, first_out):
    coarse = own_ref[...] + sub_ref[...] + grp_ref[...]
    coarse_out[...] = coarse
    first_out[...] = mm3(coarse, inverse_ref[...])


def first_step(own, sub, grp, inverse):
    shape = jax.ShapeDtypeStruct(own.shape, F32)
    return call(
        first_body,
        (shape, shape),
        flops=own.size * 128 * 6,
        moved=own.size * 24,
        in_specs=[VMEM] * 4,
        out_specs=(VMEM,) * 2,
        limit=4 * 1024 * 1024,
    )(own, sub, grp, inverse)


def merge_body(*refs):
    out_ref = refs[-1]
    for place, ref in enumerate(refs[:-1]):
        size = ref.shape[0]
        out_ref[place * size : (place + 1) * size] = ref[...]


def merge(pieces):
    size = pieces[0].shape[0]
    shape = jax.ShapeDtypeStruct((size * len(pieces),) + pieces[0].shape[1:], F32)
    return call(
        merge_body,
        shape,
        flops=1000,
        moved=shape.size * 8,
        in_specs=[VMEM] * len(pieces),
        out_specs=VMEM,
        limit=4 * 1024 * 1024,
    )(*pieces)


def correct_body(paired, pattern_ref, window_ref, beside_ref, coarse_ref, first_ref, matrix_ref, inverse_ref, local_ref, out_ref, product_ref, held_ref):
    size = window_ref.shape[0]
    held_ref[:size] = window_ref[...]
    held_ref[size:] = beside_ref[...]
    grp_count = lax.axis_size("grp")
    sub_count = lax.axis_size("sub")
    my_sub = lax.axis_index("sub")
    my_grp = lax.axis_index("grp")
    acc = None
    for k in range(matrix_ref.shape[0]):
        entry = pattern_ref[0, k]
        entry_sub = entry // grp_count
        entry_grp = entry - entry_sub * grp_count
        offset = lax.rem(entry_sub - my_sub + REACH_SUBS + sub_count, sub_count) - REACH_SUBS
        position = sub_slot(offset, my_sub, sub_count)
        if paired:
            apart = entry_grp ^ my_grp
            index = ((apart & 1) * (2 * REACH_SUBS + 1) + position) * 2 + (apart >> 1)
        else:
            index = position * grp_count + entry_grp
        term = mm3(held_ref[index], matrix_ref[k])
        acc = term if acc is None else acc + term
    coarse = coarse_ref[...]
    result = first_ref[...] + mm3(coarse - acc, inverse_ref[...])
    out_ref[...] = result
    product_ref[...] = row_sums(coarse * result) + local_ref[...]


def correct(paired, pattern, window, beside, coarse, first, matrix, inverse, local):
    shape = jax.ShapeDtypeStruct(first.shape, F32)
    return call(
        functools.partial(correct_body, paired),
        (shape, jax.ShapeDtypeStruct((8, first.shape[0]), F32)),
        flops=matrix.size * 128 * 6,
        moved=window.size * 4,
        scratch=[pltpu.VMEM((window.shape[0] + beside.shape[0],) + window.shape[1:], F32)],
        in_specs=[SMEM] + [VMEM] * 7,
        out_specs=(VMEM, VMEM),
        limit=8 * 1024 * 1024,
    )(pattern, window, beside, coarse, first, matrix, inverse, local)


def local_body(slots_ref, halved_ref, factor_ref, aux_sub_ref, aux_grp_ref, out_ref, product_ref):
    width = factor_ref.shape[1]
    half = halved_ref.shape[1] // 2
    per_face = half // width
    acc = jnp.zeros((halved_ref.shape[0], width), F32)
    for which, aux in ((1, aux_sub_ref), (3, aux_grp_ref)):
        base = (which // 2) * half
        first = slots_ref[0, which] * per_face
        for b in range(per_face):
            cols = slice(base + b * width, base + (b + 1) * width)
            halved = halved_ref[:, cols]
            high, low = split(halved)
            mine = factor_ref[first + b]
            theirs = aux[b * width : (b + 1) * width, :].astype(BF16)
            pair = jnp.concatenate([mine, theirs], 1)
            middle = mm(jnp.concatenate([high, low], 1), twice(pair, 0))
            middle_high, middle_low = split(middle)
            solved = mm(middle_high, pair, NT) + mm(middle_low, pair, NT)
            out_ref[:, cols] = solved * 0.5
            acc += halved * solved
    product_ref[...] = row_sums(acc)


def local_solve(slots, fresh, factor, aux_sub, aux_grp):
    return call(
        local_body,
        (jax.ShapeDtypeStruct(fresh.shape, F32), jax.ShapeDtypeStruct((8, fresh.shape[0]), F32)),
        flops=fresh.size * 128 * 16,
        moved=fresh.size * 12,
        in_specs=[SMEM] + [VMEM] * 4,
        out_specs=(VMEM, VMEM),
        limit=10 * 1024 * 1024,
    )(slots, fresh, factor, aux_sub, aux_grp)


def spread_body(slots_ref, solved_ref, own_ref, from_sub_ref, from_grp_ref, block_ref, basis_ref, aux_sub_ref, aux_grp_ref, iterate_ref, direction_ref, curve_ref, product_ref, out_ref, iterate_out):
    width = basis_ref.shape[1]
    prims = basis_ref.shape[0]
    half = solved_ref.shape[1] // 2
    per_face = half // width
    rows = half
    own = own_ref[...] * 0.5
    basis = basis_ref[...]
    scale = per_row(product_ref[...] / curve_ref[...], width)
    for which, aux, other_ref in ((1, aux_sub_ref, from_sub_ref), (3, aux_grp_ref, from_grp_ref)):
        base = (which // 2) * half
        both = jnp.concatenate([own, other_ref[...] * 0.5], 1)
        right = jnp.concatenate([basis, aux[rows : rows + prims, :].astype(BF16)], 0)
        own_near = (block_ref[...] - slots_ref[0, which] * per_face).astype(F32)
        near = jnp.concatenate([own_near, aux[rows + prims : rows + prims + 1, :]], 1)
        for b in range(per_face):
            cols = slice(base + b * width, base + (b + 1) * width)
            high, low = split(jnp.where(near == b, both, 0.0))
            out_ref[:, cols] = solved_ref[:, cols] + (mm(high, right) + mm(low, right))
            iterate_out[:, cols] = iterate_ref[:, cols] + scale * direction_ref[:, cols]


def spread(slots, solved, own, from_sub, from_grp, blocks, basis, aux_sub, aux_grp, iterate, direction, curve, product):
    return call(
        spread_body,
        (jax.ShapeDtypeStruct(solved.shape, F32),) * 2,
        flops=solved.size * 128 * 8,
        moved=solved.size * 12,
        in_specs=[SMEM] + [VMEM] * 12,
        out_specs=(VMEM, VMEM),
        limit=10 * 1024 * 1024,
    )(slots, solved, own, from_sub, from_grp, blocks, basis, aux_sub, aux_grp, iterate, direction, curve, product)


def shards(
    solution,
    residual,
    direction,
    residual_product,
    neighbor_slots,
    coupling,
    dirichlet_factor,
    face_block,
    neumann_factor,
    primal_block,
    primal_basis,
    coarse_matrix,
    coarse_block_inverse,
    coarse_pattern,
):
    width = face_block.shape[2]
    per_face = face_block.shape[1] // 4
    face_width = per_face * width
    own = direction[0]
    basis = primal_basis[0]
    factor = neumann_factor[0]
    product = residual_product[None, :]
    grp_count = lax.axis_size("grp")

    from_sub = shifted(own[:, :face_width], "sub", 1)
    from_grp = shifted(own[:, face_width:], "grp", 1)
    keep = (face_block[0], factor, basis, primal_block)
    couple, middle, face, factor, basis, blocks = prepare(coupling[0], dirichlet_factor[0], keep)
    aux_sub, aux_grp = pack(neighbor_slots, blocks, basis, factor, per_face)
    aux_sub, aux_grp, face = lax.optimization_barrier((aux_sub, aux_grp, face))
    aux_sub = shifted(aux_sub, "sub", -1)
    aux_grp = shifted(aux_grp, "grp", -1)
    keep = (own, residual[0], coarse_matrix[0], coarse_block_inverse[0], solution[0])
    high, low, own, old, matrix, inverse, iterate = assemble(couple, middle, face, keep)

    y, curve = apply(neighbor_slots, own, from_sub, from_grp, high, low)
    back_sub = shifted(y[0], "sub", -1)
    curve = total(curve, "grp")
    lower, curve = lax.optimization_barrier((y[2], curve))
    back_grp = shifted(lower, "grp", -1)
    curve = total(curve, "sub")
    fresh, halved, part, part_sub, part_grp = update(
        neighbor_slots, y, back_sub, back_grp, old, curve, product, blocks, basis, aux_sub, aux_grp
    )
    part_sub = shifted(part_sub, "sub", 1)
    part_grp = shifted(part_grp, "grp", 1)
    solved, local = local_solve(neighbor_slots, halved, factor, aux_sub, aux_grp)
    coarse, first = first_step(part, part_sub, part_grp, inverse)

    if grp_count == 4:
        group = jnp.stack([first, shifted(first, "grp", 2)], 0)
    else:
        group = lax.all_gather(first[None], "grp", axis=0, tiled=True)
    window = merge([group] + sub_window(group))
    beside = window[:1]
    if grp_count == 4:
        beside = lax.ppermute(window, "grp", [(i, i ^ 1) for i in range(grp_count)])

    correction, partial = correct(grp_count == 4, coarse_pattern, window, beside, coarse, first, matrix, inverse, local)
    partial = total(partial, "grp")
    sent, partial = lax.optimization_barrier((correction, partial))
    other_sub = shifted(sent, "sub", -1)
    other_grp = shifted(sent, "grp", -1)

    def late(value):
        value, first_in, second_in = lax.optimization_barrier((value, other_sub, other_grp))
        return value, spread(
            neighbor_slots, solved, correction, first_in, second_in, blocks, basis, aux_sub, aux_grp, iterate, own, curve, product
        )

    new_product, (preconditioned, new_solution) = total_with(partial, "sub", late)
    new_product = new_product[0]
    step_ratio = new_product / residual_product
    new_direction = preconditioned[None] + step_ratio[None, :, None] * own[None]
    return (new_solution[None], fresh[None], new_direction, new_product)


def solution(mesh):
    in_specs = (
        P(("sub", "grp"), None, None),
        P(("sub", "grp"), None, None),
        P(("sub", "grp"), None, None),
        P(),
        P(("sub", "grp"), None),
        P(("sub", "grp"), None, None, None),
        P(("sub", "grp"), None, None, None),
        P(("sub", "grp"), None, None, None),
        P(("sub", "grp"), None, None, None),
        P(("sub", "grp"), None),
        P(("sub", "grp"), None, None),
        P(("sub", "grp"), None, None, None),
        P(("sub", "grp"), None, None),
        P(("sub", "grp"), None),
    )
    out_specs = (
        P(("sub", "grp"), None, None),
        P(("sub", "grp"), None, None),
        P(("sub", "grp"), None, None),
        P(),
    )

    return jax.shard_map(shards, mesh=mesh, in_specs=in_specs, out_specs=out_specs, check_vma=False)
```

```python
import functools

import jax
import jax.numpy as jnp
from jax import lax
from jax.experimental import pallas as pl
from jax.experimental.pallas import tpu as pltpu
from jax.sharding import PartitionSpec as P


REACH_SUBS = 2
F32 = jnp.float32
BF16 = jnp.bfloat16
VMEM = pl.BlockSpec(memory_space=pltpu.VMEM)
SMEM = pl.BlockSpec(memory_space=pltpu.SMEM)
NN = (((1,), (0,)), ((), ()))
NT = (((1,), (1,)), ((), ()))


def shifted(value, axis, steps):
    count = lax.axis_size(axis)
    pairs = [(source, (source + steps) % count) for source in range(count)]
    return lax.ppermute(value, axis, pairs)


def total(value, axis):
    count = lax.axis_size(axis)
    if count & (count - 1):
        return lax.psum(value, axis)
    bits = [1 << k for k in range(count.bit_length() - 1)]
    for bit in reversed(bits) if axis == "sub" else bits:
        value = value + lax.ppermute(value, axis, [(i, i ^ bit) for i in range(count)])
    return value


def total_with(value, axis, late):
    count = lax.axis_size(axis)
    if count & (count - 1):
        value, extra = late(value)
        return lax.psum(value, axis), extra
    bit = 1
    extra = None
    while bit < count:
        if 2 * bit == count:
            value, extra = late(value)
        value = value + lax.ppermute(value, axis, [(i, i ^ bit) for i in range(count)])
        bit *= 2
    return value, extra


def swapped_window(count):
    return REACH_SUBS == 2 and count % 4 == 0 and count > 4


def sub_window(group):
    count = lax.axis_size("sub")
    everyone = range(count)
    if swapped_window(count):
        targets = (
            [i ^ 1 for i in everyone],
            [(i - 1 + 2 * (i & 1)) % count for i in everyone],
            [i ^ 2 for i in everyone],
            [(i - 2 + 2 * (i & 2)) % count for i in everyone],
        )
    else:
        targets = [[(i - step) % count for i in everyone] for step in range(-REACH_SUBS, REACH_SUBS + 1) if step]
    pieces = []
    for target in targets:
        pieces.append(lax.ppermute(group, "sub", list(zip(everyone, target))))
    return pieces


def sub_slot(offset, mine, count):
    if swapped_window(count):
        far = jnp.where((mine & 2 == 0) == (offset == 2), 3, 4)
        near = jnp.where((mine & 1 == 0) == (offset == 1), 1, 2)
        return jnp.where(offset == 0, 0, jnp.where((offset == 1) | (offset == -1), near, far))
    return jnp.where(offset == 0, 0, offset + REACH_SUBS + (offset < 0).astype(jnp.int32))


def split(value):
    high = value.astype(BF16)
    low = (value - high.astype(F32)).astype(BF16)
    return high, low


def mm(a, b, dims=NN):
    return lax.dot_general(a, b, dims, preferred_element_type=F32)


def mm3(a, b):
    a_high, a_low = split(a)
    b_high, b_low = split(b)
    return mm(a_high, b_high) + (mm(a_low, b_high) + mm(a_high, b_low))


def twice(value, axis):
    return jnp.concatenate([value, value], axis=axis)


def row_sums(partial):
    ones = jnp.ones((8, partial.shape[1]), F32)
    return lax.dot_general(ones, partial, NT, precision=lax.Precision.HIGHEST, preferred_element_type=F32)


def per_row(row, width):
    tall = jnp.broadcast_to(row[0:1], (width, row.shape[1]))
    return tall.T


def call(body, out_shapes, flops, moved, scratch=(), grid=None, in_specs=None, out_specs=None, limit=None):
    params = {}
    if limit is not None:
        params["vmem_limit_bytes"] = limit
    kwargs = {}
    if grid is not None:
        kwargs["grid"] = grid
    return pl.pallas_call(
        body,
        out_shape=out_shapes,
        in_specs=in_specs,
        out_specs=out_specs,
        scratch_shapes=scratch,
        compiler_params=pltpu.CompilerParams(**params),
        cost_estimate=pl.CostEstimate(flops=flops, bytes_accessed=moved, transcendentals=0),
        **kwargs,
    )


BATCH = 16


def in_hbm(value):
    return pltpu.with_memory_space_constraint(value, pltpu.HBM)


def prepare_body(kept, couple_hbm, factor_hbm, *refs):
    sources = refs[:kept]
    couple_ref, middle_ref = refs[kept : kept + 2]
    targets = refs[kept + 2 : 2 * kept + 2]
    factor_ref, inner_ref, sems, keep_sems = refs[2 * kept + 2 :]
    width = factor_ref.shape[1]
    rounds = couple_ref.shape[0] // BATCH

    def copy_of(i, which):
        part = pl.ds(i * BATCH, BATCH)
        source, target = ((factor_hbm, factor_ref), (couple_hbm, couple_ref))[which]
        return pltpu.make_async_copy(source.at[part], target.at[part], sems.at[which, i])

    def begin(i, carry):
        for which in range(2):
            copy_of(i, which).start()
        return carry

    keeping = [pltpu.make_async_copy(a, b, keep_sems.at[i]) for i, (a, b) in enumerate(zip(sources, targets))]
    lax.fori_loop(0, rounds, begin, 0)
    for copy in keeping:
        copy.start()

    def inner(i):
        for k in range(BATCH):
            factor = factor_ref[i * BATCH + k]
            high, low = split(mm(factor, factor, NT))
            inner_ref[i % 2, k, :width] = high
            inner_ref[i % 2, k, width:] = low

    def middle(i):
        for k in range(BATCH):
            high, low = split(mm(twice(couple_ref[i * BATCH + k], 1), inner_ref[i % 2, k]))
            middle_ref[i * BATCH + k, :, :width] = high
            middle_ref[i * BATCH + k, :, width:] = low

    copy_of(0, 0).wait()
    inner(0)

    def steady(i, carry):
        copy_of(i, 0).wait()
        copy_of(i - 1, 1).wait()
        inner(i)
        middle(i - 1)
        return carry

    lax.fori_loop(1, rounds, steady, 0)
    copy_of(rounds - 1, 1).wait()
    middle(rounds - 1)
    for copy in keeping:
        copy.wait()


def prepare(coupling, dirichlet, keep):
    count, double, width = coupling.shape
    hbm = pl.BlockSpec(memory_space=pltpu.HBM)
    return call(
        functools.partial(prepare_body, len(keep)),
        (
            jax.ShapeDtypeStruct(coupling.shape, BF16),
            jax.ShapeDtypeStruct((count, double, double), BF16),
        )
        + tuple(jax.ShapeDtypeStruct(k.shape, k.dtype) for k in keep),
        flops=count * 2 * width**3 * 6,
        moved=coupling.size * 3,
        scratch=[
            pltpu.VMEM((count, width, width), BF16),
            pltpu.VMEM((2, BATCH, double, width), BF16),
            pltpu.SemaphoreType.DMA((2, count // BATCH)),
            pltpu.SemaphoreType.DMA((len(keep),)),
        ],
        in_specs=[hbm] * (2 + len(keep)),
        out_specs=(VMEM,) * (2 + len(keep)),
        limit=6 * 1024 * 1024,
    )(in_hbm(coupling), in_hbm(dirichlet), *(in_hbm(k) for k in keep))


def assemble_body(blocks, kept, couple_ref, middle_ref, face_ref, *refs):
    sources = refs[:kept]
    high_ref, low_ref = refs[kept : kept + 2]
    targets = refs[kept + 2 : 2 * kept + 2]
    near_ref, far_ref, keep_sems = refs[2 * kept + 2 :]
    width = face_ref.shape[1]
    count = couple_ref.shape[0]
    reach = count // blocks
    pairs = blocks // 2
    keeping = [pltpu.make_async_copy(a, b, keep_sems.at[i]) for i, (a, b) in enumerate(zip(sources, targets))]
    for copy in keeping:
        copy.start()

    def convert(block, carry):
        near_ref[block] = face_ref[block].astype(F32)
        far_ref[block] = jnp.zeros((width, width), F32)
        return carry

    lax.fori_loop(0, blocks, convert, 0)
    for extra in range(reach):
        far_ref[blocks + extra] = jnp.zeros((width, width), F32)

    def put(pair, row, half, value):
        high, low = split(value)
        cols = pl.ds(pl.multiple_of(half * width, width), width)
        high_ref[pair, row, :, cols] = high
        low_ref[pair, row, :, cols] = low

    def outer(i, carry):
        per = blocks // BATCH
        q = i // per
        base = (i - q * per) * BATCH
        for k in range(BATCH):
            full = mm(middle_ref[i * BATCH + k], twice(couple_ref[i * BATCH + k], 1), NT)
            place = base + k
            reached = place + q + 1
            near_ref[place] += full[:width, :width]
            far_ref[reached] += full[width:, width:]
            wrapped = lax.rem(reached, blocks)
            half = lax.rem(wrapped, 2)
            put(wrapped // 2, reach - 1 - q + half, half, full[:width, width:])
            side = k % 2
            put(place // 2, reach + q + 1 + side, side, full[width:, :width])
        return carry

    lax.fori_loop(0, count // BATCH, outer, 0)

    def close(pair, carry):
        zero = jnp.zeros((width, width), BF16)
        for ref in (high_ref, low_ref):
            ref[pair, 2 * reach + 1, :, pl.ds(0, width)] = zero
            ref[pair, 0, :, pl.ds(width, width)] = zero
        for side in range(2):
            put(pair, reach + side, side, near_ref[2 * pair + side] + far_ref[2 * pair + side])
        return carry

    for extra in range(reach):
        far_ref[extra] += far_ref[blocks + extra]
    lax.fori_loop(0, pairs, close, 0)
    for copy in keeping:
        copy.wait()


def assemble(couple, middle, face, keep):
    blocks, width, _ = face.shape
    count = couple.shape[0]
    reach = count // blocks
    pairs = blocks // 2
    shape = jax.ShapeDtypeStruct((pairs, 2 * reach + 2, width, 2 * width), BF16)
    hbm = pl.BlockSpec(memory_space=pltpu.HBM)
    return call(
        functools.partial(assemble_body, blocks, len(keep)),
        (shape, shape) + tuple(jax.ShapeDtypeStruct(k.shape, k.dtype) for k in keep),
        flops=count * 2 * width**3 * 6,
        moved=couple.size * 3,
        scratch=[
            pltpu.VMEM((blocks, width, width), F32),
            pltpu.VMEM((blocks + reach, width, width), F32),
            pltpu.SemaphoreType.DMA((len(keep),)),
        ],
        in_specs=[VMEM] * 3 + [hbm] * len(keep),
        out_specs=(VMEM,) * (2 + len(keep)),
        limit=6 * 1024 * 1024,
    )(couple, middle, face, *(in_hbm(k) for k in keep))


def apply_body(slots_ref, own_ref, from_sub_ref, from_grp_ref, high_ref, low_ref, out_ref, curve_ref, u_high, u_low):
    pairs, count, width, _ = high_ref.shape
    reach = count // 2 - 1
    face_width = from_sub_ref.shape[1]
    per_face = face_width // width
    blocks = 2 * pairs
    loads = own_ref.shape[0]
    faces = ((from_sub_ref, 0), (own_ref, 0), (from_grp_ref, 0), (own_ref, face_width))
    for which, (ref, base) in enumerate(faces):
        slot = slots_ref[0, which]
        for b in range(per_face):
            high, low = split(ref[:, base + b * width : base + (b + 1) * width])
            place = slot * per_face + b + reach
            u_high[place] = high
            u_low[place] = low
    for ref in (u_high, u_low):
        for i in range(reach):
            ref[i] = ref[blocks + i]
        for i in range(reach + 1):
            ref[blocks + reach + i] = ref[reach + i]
    half_face = per_face // 2

    def one_face(which, carry):
        slot = slots_ref[0, which]
        for part in range(half_face):
            pair = slot * half_face + part
            high = jnp.concatenate([u_high[2 * pair + i] for i in range(count)], 1)
            low = jnp.concatenate([u_low[2 * pair + i] for i in range(count)], 1)
            weight = high_ref[pair].reshape(count * width, 2 * width)
            both = mm(jnp.concatenate([high, low], 0), weight)
            result = both[:loads] + both[loads:] + mm(high, low_ref[pair].reshape(count * width, 2 * width))
            out_ref[which, :, part * 2 * width : (part + 1) * 2 * width] = result
        return carry

    lax.fori_loop(0, 4, one_face, 0)
    acc = jnp.zeros((loads, width), F32)
    for which, (ref, base) in enumerate(faces):
        for b in range(per_face):
            acc += ref[:, base + b * width : base + (b + 1) * width] * out_ref[which, :, b * width : (b + 1) * width]
    curve_ref[...] = row_sums(acc)


def apply(slots, own, from_sub, from_grp, high, low):
    pairs, count, width, _ = high.shape
    loads, face_width = from_sub.shape
    return call(
        apply_body,
        (
            jax.ShapeDtypeStruct((4, loads, face_width), F32),
            jax.ShapeDtypeStruct((8, loads), F32),
        ),
        flops=high.size * loads * 6,
        moved=high.size * 4,
        scratch=[pltpu.VMEM((2 * pairs + count - 1, loads, width), BF16)] * 2,
        in_specs=[SMEM] + [VMEM] * 5,
        out_specs=(VMEM, VMEM),
        limit=6 * 1024 * 1024,
    )(slots, own, from_sub, from_grp, high, low)


def pack_body(per_face, slots_ref, block_ref, basis_ref, factor_ref, sub_ref, grp_ref):
    prims, width = basis_ref.shape
    rows = per_face * width
    for out, which in ((sub_ref, 0), (grp_ref, 2)):
        first = slots_ref[0, which] * per_face
        for b in range(per_face):
            out[b * width : (b + 1) * width, :] = factor_ref[first + b].astype(F32)
        out[rows : rows + prims, :] = basis_ref[...].astype(F32)
        near = (block_ref[...] - first).astype(F32)
        out[rows + prims :, :] = jnp.broadcast_to(near, (8, width))


def pack(slots, blocks, basis, factor, per_face):
    prims, width = basis.shape
    shape = jax.ShapeDtypeStruct((per_face * width + prims + 8, width), F32)
    return call(
        functools.partial(pack_body, per_face),
        (shape, shape),
        flops=1000,
        moved=shape.size * 12,
        in_specs=[SMEM] + [VMEM] * 3,
        out_specs=(VMEM, VMEM),
        limit=4 * 1024 * 1024,
    )(slots, blocks, basis, factor)


def image_body(slots_ref, y_ref, back_sub_ref, back_grp_ref, residual_ref, block_ref, basis_ref, aux_sub_ref, aux_grp_ref, image_out, own_out, sub_out, grp_out):
    prims, width = basis_ref.shape
    face_width = back_sub_ref.shape[1]
    per_face = face_width // width
    rows = face_width
    loads = residual_ref.shape[0]
    basis = basis_ref[...].astype(F32).T
    own_total = None
    for which, back, aux, out in (
        (1, back_sub_ref, aux_sub_ref, sub_out),
        (3, back_grp_ref, aux_grp_ref, grp_out),
    ):
        offset = (which // 2) * face_width
        other = aux[rows : rows + prims, :].T
        own_near = block_ref[...] - slots_ref[0, which] * per_face
        other_near = aux[rows + prims : rows + prims + 1, :]
        both = None
        for b in range(per_face):
            cols = slice(b * width, (b + 1) * width)
            wide = slice(offset + b * width, offset + (b + 1) * width)
            image = y_ref[which, :, cols] + back[:, cols]
            image_out[:, wide] = image
            image_high, image_low = split(image)
            high, low = split(residual_ref[:, wide])
            left = jnp.concatenate(
                [jnp.concatenate([image_high, image_low], 1), jnp.concatenate([high, low], 1)], 0
            )
            mine = jnp.where(own_near == b, basis, 0.0).astype(BF16)
            theirs = jnp.where(other_near == b, other, 0.0).astype(BF16)
            term = mm(left, twice(jnp.concatenate([mine, theirs], 1), 0))
            both = term if both is None else both + term
        own = both[:, :prims]
        own_total = own if own_total is None else own_total + own
        out[0] = both[:loads, prims:] * 0.5
        out[1] = both[loads:, prims:] * 0.5
    own_out[0] = own_total[:loads] * 0.5
    own_out[1] = own_total[loads:] * 0.5


def find_image(slots, y, back_sub, back_grp, residual, blocks, basis, aux_sub, aux_grp):
    loads = residual.shape[0]
    prims = basis.shape[0]
    small = jax.ShapeDtypeStruct((2, loads, prims), F32)
    return call(
        image_body,
        (jax.ShapeDtypeStruct(residual.shape, F32), small, small, small),
        flops=residual.size * prims * 16,
        moved=residual.size * 20,
        in_specs=[SMEM] + [VMEM] * 8,
        out_specs=(VMEM,) * 4,
        limit=8 * 1024 * 1024,
    )(slots, y, back_sub, back_grp, residual, blocks, basis, aux_sub, aux_grp)


def advance_body(image_ref, residual_ref, curve_ref, product_ref, residual_out, half_out):
    width = curve_ref.shape[1]
    scale = per_row(product_ref[...] / curve_ref[...], width)
    for b in range(image_ref.shape[1] // width):
        cols = slice(b * width, (b + 1) * width)
        fresh = residual_ref[:, cols] - scale * image_ref[:, cols]
        residual_out[:, cols] = fresh
        half_out[:, cols] = fresh * 0.5


def advance(image, residual, curve, product):
    shape = jax.ShapeDtypeStruct(residual.shape, F32)
    return call(
        advance_body,
        (shape, shape),
        flops=residual.size * 400,
        moved=residual.size * 16,
        in_specs=[VMEM] * 4,
        out_specs=(VMEM,) * 2,
        limit=4 * 1024 * 1024,
    )(image, residual, curve, product)


def first_body(own_ref, sub_ref, grp_ref, curve_ref, product_ref, inverse_ref, coarse_out, first_out):
    scale = per_row(product_ref[...] / curve_ref[...], own_ref.shape[2])
    parts = own_ref[...] + sub_ref[...] + grp_ref[...]
    coarse = parts[1] - scale * parts[0]
    coarse_out[...] = coarse
    first_out[...] = mm3(coarse, inverse_ref[...])


def first_step(own, sub, grp, curve, product, inverse):
    shape = jax.ShapeDtypeStruct(own.shape[1:], F32)
    return call(
        first_body,
        (shape, shape),
        flops=own.size * 128 * 6,
        moved=own.size * 24,
        in_specs=[VMEM] * 6,
        out_specs=(VMEM,) * 2,
        limit=4 * 1024 * 1024,
    )(own, sub, grp, curve, product, inverse)


def merge_body(*refs):
    out_ref = refs[-1]
    for place, ref in enumerate(refs[:-1]):
        size = ref.shape[0]
        out_ref[place * size : (place + 1) * size] = ref[...]


def merge(pieces):
    size = pieces[0].shape[0]
    shape = jax.ShapeDtypeStruct((size * len(pieces),) + pieces[0].shape[1:], F32)
    return call(
        merge_body,
        shape,
        flops=1000,
        moved=shape.size * 8,
        in_specs=[VMEM] * len(pieces),
        out_specs=VMEM,
        limit=4 * 1024 * 1024,
    )(*pieces)


def correct_body(paired, pattern_ref, window_ref, beside_ref, coarse_ref, first_ref, matrix_ref, inverse_ref, local_ref, out_ref, product_ref, held_ref):
    size = window_ref.shape[0]
    held_ref[:size] = window_ref[...]
    held_ref[size:] = beside_ref[...]
    grp_count = lax.axis_size("grp")
    sub_count = lax.axis_size("sub")
    my_sub = lax.axis_index("sub")
    my_grp = lax.axis_index("grp")
    acc = None
    for k in range(matrix_ref.shape[0]):
        entry = pattern_ref[0, k]
        entry_sub = entry // grp_count
        entry_grp = entry - entry_sub * grp_count
        offset = lax.rem(entry_sub - my_sub + REACH_SUBS + sub_count, sub_count) - REACH_SUBS
        position = sub_slot(offset, my_sub, sub_count)
        if paired:
            apart = entry_grp ^ my_grp
            index = ((apart & 1) * (2 * REACH_SUBS + 1) + position) * 2 + (apart >> 1)
        else:
            index = position * grp_count + entry_grp
        term = mm3(held_ref[index], matrix_ref[k])
        acc = term if acc is None else acc + term
    coarse = coarse_ref[...]
    result = first_ref[...] + mm3(coarse - acc, inverse_ref[...])
    out_ref[...] = result
    product_ref[...] = row_sums(coarse * result) + local_ref[...]


def correct(paired, pattern, window, beside, coarse, first, matrix, inverse, local):
    shape = jax.ShapeDtypeStruct(first.shape, F32)
    return call(
        functools.partial(correct_body, paired),
        (shape, jax.ShapeDtypeStruct((8, first.shape[0]), F32)),
        flops=matrix.size * 128 * 6,
        moved=window.size * 4,
        scratch=[pltpu.VMEM((window.shape[0] + beside.shape[0],) + window.shape[1:], F32)],
        in_specs=[SMEM] + [VMEM] * 7,
        out_specs=(VMEM, VMEM),
        limit=8 * 1024 * 1024,
    )(pattern, window, beside, coarse, first, matrix, inverse, local)


def local_body(slots_ref, halved_ref, factor_ref, aux_sub_ref, aux_grp_ref, out_ref, product_ref):
    width = factor_ref.shape[1]
    half = halved_ref.shape[1] // 2
    per_face = half // width
    acc = jnp.zeros((halved_ref.shape[0], width), F32)
    for which, aux in ((1, aux_sub_ref), (3, aux_grp_ref)):
        base = (which // 2) * half
        first = slots_ref[0, which] * per_face
        for b in range(per_face):
            cols = slice(base + b * width, base + (b + 1) * width)
            halved = halved_ref[:, cols]
            high, low = split(halved)
            mine = factor_ref[first + b]
            theirs = aux[b * width : (b + 1) * width, :].astype(BF16)
            pair = jnp.concatenate([mine, theirs], 1)
            middle = mm(jnp.concatenate([high, low], 1), twice(pair, 0))
            middle_high, middle_low = split(middle)
            solved = mm(middle_high, pair, NT) + mm(middle_low, pair, NT)
            out_ref[:, cols] = solved * 0.5
            acc += halved * solved
    product_ref[...] = row_sums(acc)


def local_solve(slots, fresh, factor, aux_sub, aux_grp):
    return call(
        local_body,
        (jax.ShapeDtypeStruct(fresh.shape, F32), jax.ShapeDtypeStruct((8, fresh.shape[0]), F32)),
        flops=fresh.size * 128 * 16,
        moved=fresh.size * 12,
        in_specs=[SMEM] + [VMEM] * 4,
        out_specs=(VMEM, VMEM),
        limit=10 * 1024 * 1024,
    )(slots, fresh, factor, aux_sub, aux_grp)


def spread_body(slots_ref, solved_ref, own_ref, from_sub_ref, from_grp_ref, block_ref, basis_ref, aux_sub_ref, aux_grp_ref, iterate_ref, direction_ref, curve_ref, product_ref, out_ref, iterate_out):
    width = basis_ref.shape[1]
    prims = basis_ref.shape[0]
    half = solved_ref.shape[1] // 2
    per_face = half // width
    rows = half
    own = own_ref[...] * 0.5
    basis = basis_ref[...]
    scale = per_row(product_ref[...] / curve_ref[...], width)
    for which, aux, other_ref in ((1, aux_sub_ref, from_sub_ref), (3, aux_grp_ref, from_grp_ref)):
        base = (which // 2) * half
        both = jnp.concatenate([own, other_ref[...] * 0.5], 1)
        right = jnp.concatenate([basis, aux[rows : rows + prims, :].astype(BF16)], 0)
        own_near = (block_ref[...] - slots_ref[0, which] * per_face).astype(F32)
        near = jnp.concatenate([own_near, aux[rows + prims : rows + prims + 1, :]], 1)
        for b in range(per_face):
            cols = slice(base + b * width, base + (b + 1) * width)
            high, low = split(jnp.where(near == b, both, 0.0))
            out_ref[:, cols] = solved_ref[:, cols] + (mm(high, right) + mm(low, right))
            iterate_out[:, cols] = iterate_ref[:, cols] + scale * direction_ref[:, cols]


def spread(slots, solved, own, from_sub, from_grp, blocks, basis, aux_sub, aux_grp, iterate, direction, curve, product):
    return call(
        spread_body,
        (jax.ShapeDtypeStruct(solved.shape, F32),) * 2,
        flops=solved.size * 128 * 8,
        moved=solved.size * 12,
        in_specs=[SMEM] + [VMEM] * 12,
        out_specs=(VMEM, VMEM),
        limit=10 * 1024 * 1024,
    )(slots, solved, own, from_sub, from_grp, blocks, basis, aux_sub, aux_grp, iterate, direction, curve, product)


def shards(
    solution,
    residual,
    direction,
    residual_product,
    neighbor_slots,
    coupling,
    dirichlet_factor,
    face_block,
    neumann_factor,
    primal_block,
    primal_basis,
    coarse_matrix,
    coarse_block_inverse,
    coarse_pattern,
):
    width = face_block.shape[2]
    per_face = face_block.shape[1] // 4
    face_width = per_face * width
    own = direction[0]
    basis = primal_basis[0]
    factor = neumann_factor[0]
    product = residual_product[None, :]
    grp_count = lax.axis_size("grp")

    from_sub = shifted(own[:, :face_width], "sub", 1)
    from_grp = shifted(own[:, face_width:], "grp", 1)
    keep = (face_block[0], factor, basis, primal_block)
    couple, middle, face, factor, basis, blocks = prepare(coupling[0], dirichlet_factor[0], keep)
    aux_sub, aux_grp = pack(neighbor_slots, blocks, basis, factor, per_face)
    aux_sub, aux_grp, face = lax.optimization_barrier((aux_sub, aux_grp, face))
    aux_sub = shifted(aux_sub, "sub", -1)
    aux_grp = shifted(aux_grp, "grp", -1)
    keep = (own, residual[0], coarse_matrix[0], coarse_block_inverse[0], solution[0])
    high, low, own, old, matrix, inverse, iterate = assemble(couple, middle, face, keep)

    y, curve = apply(neighbor_slots, own, from_sub, from_grp, high, low)
    back_sub = shifted(y[0], "sub", -1)
    curve = total(curve, "grp")
    lower, curve = lax.optimization_barrier((y[2], curve))
    back_grp = shifted(lower, "grp", -1)
    curve = total(curve, "sub")
    image, part, part_sub, part_grp = find_image(
        neighbor_slots, y, back_sub, back_grp, old, blocks, basis, aux_sub, aux_grp
    )
    part_sub = shifted(part_sub, "sub", 1)
    part_grp = shifted(part_grp, "grp", 1)
    coarse, first = first_step(part, part_sub, part_grp, curve, product, inverse)
    fresh, halved = advance(image, old, curve, product)
    solved, local = local_solve(neighbor_slots, halved, factor, aux_sub, aux_grp)

    if grp_count == 4:
        beyond = shifted(first, "grp", 2)
        group = jnp.stack([first, beyond], 0)
    else:
        group = lax.all_gather(first[None], "grp", axis=0, tiled=True)
    window = merge([group] + sub_window(group))
    beside = window[:1]
    if grp_count == 4:
        beside = lax.ppermute(window, "grp", [(i, i ^ 1) for i in range(grp_count)])

    correction, partial = correct(grp_count == 4, coarse_pattern, window, beside, coarse, first, matrix, inverse, local)
    partial = total(partial, "grp")
    sent, partial = lax.optimization_barrier((correction, partial))
    other_sub = shifted(sent, "sub", -1)
    other_grp = shifted(sent, "grp", -1)

    def late(value):
        value, first_in, second_in = lax.optimization_barrier((value, other_sub, other_grp))
        return value, spread(
            neighbor_slots, solved, correction, first_in, second_in, blocks, basis, aux_sub, aux_grp, iterate, own, curve, product
        )

    new_product, (preconditioned, new_solution) = total_with(partial, "sub", late)
    new_product = new_product[0]
    step_ratio = new_product / residual_product
    new_direction = preconditioned[None] + step_ratio[None, :, None] * own[None]
    return (new_solution[None], fresh[None], new_direction, new_product)


def solution(mesh):
    in_specs = (
        P(("sub", "grp"), None, None),
        P(("sub", "grp"), None, None),
        P(("sub", "grp"), None, None),
        P(),
        P(("sub", "grp"), None),
        P(("sub", "grp"), None, None, None),
        P(("sub", "grp"), None, None, None),
        P(("sub", "grp"), None, None, None),
        P(("sub", "grp"), None, None, None),
        P(("sub", "grp"), None),
        P(("sub", "grp"), None, None),
        P(("sub", "grp"), None, None, None),
        P(("sub", "grp"), None, None),
        P(("sub", "grp"), None),
    )
    out_specs = (
        P(("sub", "grp"), None, None),
        P(("sub", "grp"), None, None),
        P(("sub", "grp"), None, None),
        P(),
    )

    return jax.shard_map(shards, mesh=mesh, in_specs=in_specs, out_specs=out_specs, check_vma=False)
```

```python
import functools

import jax
import jax.numpy as jnp
from jax import lax
from jax.experimental import pallas as pl
from jax.experimental.pallas import tpu as pltpu
from jax.sharding import PartitionSpec as P


REACH_SUBS = 2
F32 = jnp.float32
BF16 = jnp.bfloat16
VMEM = pl.BlockSpec(memory_space=pltpu.VMEM)
SMEM = pl.BlockSpec(memory_space=pltpu.SMEM)
NN = (((1,), (0,)), ((), ()))
NT = (((1,), (1,)), ((), ()))


def shifted(value, axis, steps):
    count = lax.axis_size(axis)
    pairs = [(source, (source + steps) % count) for source in range(count)]
    return lax.ppermute(value, axis, pairs)


def total(value, axis):
    count = lax.axis_size(axis)
    if count & (count - 1):
        return lax.psum(value, axis)
    bits = [1 << k for k in range(count.bit_length() - 1)]
    for bit in reversed(bits) if axis == "sub" else bits:
        value = value + lax.ppermute(value, axis, [(i, i ^ bit) for i in range(count)])
    return value


def total_with(value, axis, late):
    count = lax.axis_size(axis)
    if count & (count - 1):
        value, extra = late(value)
        return lax.psum(value, axis), extra
    bit = 1
    extra = None
    while bit < count:
        if 2 * bit == count:
            value, extra = late(value)
        value = value + lax.ppermute(value, axis, [(i, i ^ bit) for i in range(count)])
        bit *= 2
    return value, extra


def swapped_window(count):
    return REACH_SUBS == 2 and count % 4 == 0 and count > 4


def sub_window(group):
    count = lax.axis_size("sub")
    everyone = range(count)
    if swapped_window(count):
        targets = (
            [i ^ 1 for i in everyone],
            [(i - 1 + 2 * (i & 1)) % count for i in everyone],
            [i ^ 2 for i in everyone],
            [(i - 2 + 2 * (i & 2)) % count for i in everyone],
        )
    else:
        targets = [[(i - step) % count for i in everyone] for step in range(-REACH_SUBS, REACH_SUBS + 1) if step]
    pieces = []
    for target in targets:
        pieces.append(lax.ppermute(group, "sub", list(zip(everyone, target))))
    return pieces


def sub_slot(offset, mine, count):
    if swapped_window(count):
        far = jnp.where((mine & 2 == 0) == (offset == 2), 3, 4)
        near = jnp.where((mine & 1 == 0) == (offset == 1), 1, 2)
        return jnp.where(offset == 0, 0, jnp.where((offset == 1) | (offset == -1), near, far))
    return jnp.where(offset == 0, 0, offset + REACH_SUBS + (offset < 0).astype(jnp.int32))


def split(value):
    high = value.astype(BF16)
    low = (value - high.astype(F32)).astype(BF16)
    return high, low


def mm(a, b, dims=NN):
    return lax.dot_general(a, b, dims, preferred_element_type=F32)


def mm3(a, b):
    a_high, a_low = split(a)
    b_high, b_low = split(b)
    return mm(a_high, b_high) + (mm(a_low, b_high) + mm(a_high, b_low))


def twice(value, axis):
    return jnp.concatenate([value, value], axis=axis)


def row_sums(partial):
    ones = jnp.ones((8, partial.shape[1]), F32)
    return lax.dot_general(ones, partial, NT, precision=lax.Precision.HIGHEST, preferred_element_type=F32)


def per_row(row, width):
    tall = jnp.broadcast_to(row[0:1], (width, row.shape[1]))
    return tall.T


def call(body, out_shapes, flops, moved, scratch=(), grid=None, in_specs=None, out_specs=None, limit=None):
    params = {}
    if limit is not None:
        params["vmem_limit_bytes"] = limit
    kwargs = {}
    if grid is not None:
        kwargs["grid"] = grid
    return pl.pallas_call(
        body,
        out_shape=out_shapes,
        in_specs=in_specs,
        out_specs=out_specs,
        scratch_shapes=scratch,
        compiler_params=pltpu.CompilerParams(**params),
        cost_estimate=pl.CostEstimate(flops=flops, bytes_accessed=moved, transcendentals=0),
        **kwargs,
    )


BATCH = 16
LAST_BATCH = 32


def in_hbm(value):
    return pltpu.with_memory_space_constraint(value, pltpu.HBM)


def prepare_body(kept, couple_hbm, factor_hbm, *refs):
    sources = refs[:kept]
    couple_ref, middle_ref = refs[kept : kept + 2]
    targets = refs[kept + 2 : 2 * kept + 2]
    factor_ref, inner_ref, sems, keep_sems = refs[2 * kept + 2 :]
    width = factor_ref.shape[1]
    rounds = couple_ref.shape[0] // BATCH

    def copy_of(i, which):
        part = pl.ds(i * BATCH, BATCH)
        source, target = ((factor_hbm, factor_ref), (couple_hbm, couple_ref))[which]
        return pltpu.make_async_copy(source.at[part], target.at[part], sems.at[which, i])

    def begin(i, carry):
        for which in range(2):
            copy_of(i, which).start()
        return carry

    keeping = [pltpu.make_async_copy(a, b, keep_sems.at[i]) for i, (a, b) in enumerate(zip(sources, targets))]
    lax.fori_loop(0, rounds, begin, 0)
    for copy in keeping:
        copy.start()

    def inner(i):
        for k in range(BATCH):
            factor = factor_ref[i * BATCH + k]
            high, low = split(mm(factor, factor, NT))
            inner_ref[i % 2, k, :width] = high
            inner_ref[i % 2, k, width:] = low

    def middle(i):
        for k in range(BATCH):
            high, low = split(mm(twice(couple_ref[i * BATCH + k], 1), inner_ref[i % 2, k]))
            middle_ref[i * BATCH + k, :, :width] = high
            middle_ref[i * BATCH + k, :, width:] = low

    copy_of(0, 0).wait()
    inner(0)

    def steady(i, carry):
        copy_of(i, 0).wait()
        copy_of(i - 1, 1).wait()
        inner(i)
        middle(i - 1)
        return carry

    lax.fori_loop(1, rounds, steady, 0)
    copy_of(rounds - 1, 1).wait()
    middle(rounds - 1)
    for copy in keeping:
        copy.wait()


def prepare(coupling, dirichlet, keep):
    count, double, width = coupling.shape
    hbm = pl.BlockSpec(memory_space=pltpu.HBM)
    return call(
        functools.partial(prepare_body, len(keep)),
        (
            jax.ShapeDtypeStruct(coupling.shape, BF16),
            jax.ShapeDtypeStruct((count, double, double), BF16),
        )
        + tuple(jax.ShapeDtypeStruct(k.shape, k.dtype) for k in keep),
        flops=count * 2 * width**3 * 6,
        moved=coupling.size * 3,
        scratch=[
            pltpu.VMEM((count, width, width), BF16),
            pltpu.VMEM((2, BATCH, double, width), BF16),
            pltpu.SemaphoreType.DMA((2, count // BATCH)),
            pltpu.SemaphoreType.DMA((len(keep),)),
        ],
        in_specs=[hbm] * (2 + len(keep)),
        out_specs=(VMEM,) * (2 + len(keep)),
        limit=6 * 1024 * 1024,
    )(in_hbm(coupling), in_hbm(dirichlet), *(in_hbm(k) for k in keep))


def assemble_body(blocks, kept, couple_ref, middle_ref, face_ref, *refs):
    sources = refs[:kept]
    high_ref, low_ref = refs[kept : kept + 2]
    targets = refs[kept + 2 : 2 * kept + 2]
    near_ref, far_ref, keep_sems = refs[2 * kept + 2 :]
    width = face_ref.shape[1]
    count = couple_ref.shape[0]
    reach = count // blocks
    pairs = blocks // 2
    keeping = [pltpu.make_async_copy(a, b, keep_sems.at[i]) for i, (a, b) in enumerate(zip(sources, targets))]
    for copy in keeping:
        copy.start()

    def convert(block, carry):
        near_ref[block] = face_ref[block].astype(F32)
        far_ref[block] = jnp.zeros((width, width), F32)
        return carry

    lax.fori_loop(0, blocks, convert, 0)
    for extra in range(reach):
        far_ref[blocks + extra] = jnp.zeros((width, width), F32)

    def put(pair, row, half, value):
        high, low = split(value)
        cols = pl.ds(pl.multiple_of(half * width, width), width)
        high_ref[pair, row, :, cols] = high
        low_ref[pair, row, :, cols] = low

    def outer(i, carry):
        per = blocks // LAST_BATCH
        q = i // per
        base = (i - q * per) * LAST_BATCH
        for k in range(LAST_BATCH):
            full = mm(middle_ref[i * LAST_BATCH + k], twice(couple_ref[i * LAST_BATCH + k], 1), NT)
            place = base + k
            reached = place + q + 1
            near_ref[place] += full[:width, :width]
            far_ref[reached] += full[width:, width:]
            wrapped = lax.rem(reached, blocks)
            half = lax.rem(wrapped, 2)
            put(wrapped // 2, reach - 1 - q + half, half, full[:width, width:])
            side = k % 2
            put(place // 2, reach + q + 1 + side, side, full[width:, :width])
        return carry

    lax.fori_loop(0, count // LAST_BATCH, outer, 0)

    def close(pair, carry):
        zero = jnp.zeros((width, width), BF16)
        for ref in (high_ref, low_ref):
            ref[pair, 2 * reach + 1, :, pl.ds(0, width)] = zero
            ref[pair, 0, :, pl.ds(width, width)] = zero
        for side in range(2):
            put(pair, reach + side, side, near_ref[2 * pair + side] + far_ref[2 * pair + side])
        return carry

    for extra in range(reach):
        far_ref[extra] += far_ref[blocks + extra]
    lax.fori_loop(0, pairs, close, 0)
    for copy in keeping:
        copy.wait()


def assemble(couple, middle, face, keep):
    blocks, width, _ = face.shape
    count = couple.shape[0]
    reach = count // blocks
    pairs = blocks // 2
    shape = jax.ShapeDtypeStruct((pairs, 2 * reach + 2, width, 2 * width), BF16)
    hbm = pl.BlockSpec(memory_space=pltpu.HBM)
    return call(
        functools.partial(assemble_body, blocks, len(keep)),
        (shape, shape) + tuple(jax.ShapeDtypeStruct(k.shape, k.dtype) for k in keep),
        flops=count * 2 * width**3 * 6,
        moved=couple.size * 3,
        scratch=[
            pltpu.VMEM((blocks, width, width), F32),
            pltpu.VMEM((blocks + reach, width, width), F32),
            pltpu.SemaphoreType.DMA((len(keep),)),
        ],
        in_specs=[VMEM] * 3 + [hbm] * len(keep),
        out_specs=(VMEM,) * (2 + len(keep)),
        limit=6 * 1024 * 1024,
    )(couple, middle, face, *(in_hbm(k) for k in keep))


def apply_body(slots_ref, own_ref, from_sub_ref, from_grp_ref, high_ref, low_ref, out_ref, curve_ref, u_high, u_low):
    pairs, count, width, _ = high_ref.shape
    reach = count // 2 - 1
    face_width = from_sub_ref.shape[1]
    per_face = face_width // width
    blocks = 2 * pairs
    loads = own_ref.shape[0]
    faces = ((from_sub_ref, 0), (own_ref, 0), (from_grp_ref, 0), (own_ref, face_width))
    for which, (ref, base) in enumerate(faces):
        slot = slots_ref[0, which]
        for b in range(per_face):
            high, low = split(ref[:, base + b * width : base + (b + 1) * width])
            place = slot * per_face + b + reach
            u_high[place] = high
            u_low[place] = low
    for ref in (u_high, u_low):
        for i in range(reach):
            ref[i] = ref[blocks + i]
        for i in range(reach + 1):
            ref[blocks + reach + i] = ref[reach + i]
    half_face = per_face // 2

    acc = jnp.zeros((loads, width), F32)
    for which, (ref, base) in enumerate(faces):
        slot = slots_ref[0, which]
        for part in range(half_face):
            pair = slot * half_face + part
            high = jnp.concatenate([u_high[2 * pair + i] for i in range(count)], 1)
            low = jnp.concatenate([u_low[2 * pair + i] for i in range(count)], 1)
            weight = high_ref[pair].reshape(count * width, 2 * width)
            both = mm(jnp.concatenate([high, low], 0), weight)
            result = both[:loads] + both[loads:] + mm(high, low_ref[pair].reshape(count * width, 2 * width))
            first = 2 * part * width
            out_ref[which, :, first : first + 2 * width] = result
            acc += ref[:, base + first : base + first + width] * result[:, :width]
            acc += ref[:, base + first + width : base + first + 2 * width] * result[:, width:]
    curve_ref[...] = row_sums(acc)


def apply(slots, own, from_sub, from_grp, high, low):
    pairs, count, width, _ = high.shape
    loads, face_width = from_sub.shape
    return call(
        apply_body,
        (
            jax.ShapeDtypeStruct((4, loads, face_width), F32),
            jax.ShapeDtypeStruct((8, loads), F32),
        ),
        flops=high.size * loads * 6,
        moved=high.size * 4,
        scratch=[pltpu.VMEM((2 * pairs + count - 1, loads, width), BF16)] * 2,
        in_specs=[SMEM] + [VMEM] * 5,
        out_specs=(VMEM, VMEM),
        limit=6 * 1024 * 1024,
    )(slots, own, from_sub, from_grp, high, low)


def pack_body(per_face, slots_ref, block_ref, basis_ref, factor_ref, sub_ref, grp_ref):
    prims, width = basis_ref.shape
    rows = per_face * width
    for out, which in ((sub_ref, 0), (grp_ref, 2)):
        first = slots_ref[0, which] * per_face
        for b in range(per_face):
            out[b * width : (b + 1) * width, :] = factor_ref[first + b].astype(F32)
        out[rows : rows + prims, :] = basis_ref[...].astype(F32)
        near = (block_ref[...] - first).astype(F32)
        out[rows + prims :, :] = jnp.broadcast_to(near, (8, width))


def pack(slots, blocks, basis, factor, per_face):
    prims, width = basis.shape
    shape = jax.ShapeDtypeStruct((per_face * width + prims + 8, width), F32)
    return call(
        functools.partial(pack_body, per_face),
        (shape, shape),
        flops=1000,
        moved=shape.size * 12,
        in_specs=[SMEM] + [VMEM] * 3,
        out_specs=(VMEM, VMEM),
        limit=4 * 1024 * 1024,
    )(slots, blocks, basis, factor)


def image_body(slots_ref, y_ref, back_sub_ref, back_grp_ref, residual_ref, block_ref, basis_ref, aux_sub_ref, aux_grp_ref, image_out, own_out, sub_out, grp_out):
    prims, width = basis_ref.shape
    face_width = back_sub_ref.shape[1]
    per_face = face_width // width
    rows = face_width
    loads = residual_ref.shape[0]
    basis = basis_ref[...].astype(F32).T
    own_total = None
    for which, back, aux, out in (
        (1, back_sub_ref, aux_sub_ref, sub_out),
        (3, back_grp_ref, aux_grp_ref, grp_out),
    ):
        offset = (which // 2) * face_width
        other = aux[rows : rows + prims, :].T
        own_near = block_ref[...] - slots_ref[0, which] * per_face
        other_near = aux[rows + prims : rows + prims + 1, :]
        both = None
        for b in range(per_face):
            cols = slice(b * width, (b + 1) * width)
            wide = slice(offset + b * width, offset + (b + 1) * width)
            image = y_ref[which, :, cols] + back[:, cols]
            image_out[:, wide] = image
            image_high, image_low = split(image)
            high, low = split(residual_ref[:, wide])
            left = jnp.concatenate(
                [jnp.concatenate([image_high, image_low], 1), jnp.concatenate([high, low], 1)], 0
            )
            mine = jnp.where(own_near == b, basis, 0.0).astype(BF16)
            theirs = jnp.where(other_near == b, other, 0.0).astype(BF16)
            term = mm(left, twice(jnp.concatenate([mine, theirs], 1), 0))
            both = term if both is None else both + term
        own = both[:, :prims]
        own_total = own if own_total is None else own_total + own
        out[0] = both[:loads, prims:] * 0.5
        out[1] = both[loads:, prims:] * 0.5
    own_out[0] = own_total[:loads] * 0.5
    own_out[1] = own_total[loads:] * 0.5


def find_image(slots, y, back_sub, back_grp, residual, blocks, basis, aux_sub, aux_grp):
    loads = residual.shape[0]
    prims = basis.shape[0]
    small = jax.ShapeDtypeStruct((2, loads, prims), F32)
    return call(
        image_body,
        (jax.ShapeDtypeStruct(residual.shape, F32), small, small, small),
        flops=residual.size * prims * 16,
        moved=residual.size * 20,
        in_specs=[SMEM] + [VMEM] * 8,
        out_specs=(VMEM,) * 4,
        limit=8 * 1024 * 1024,
    )(slots, y, back_sub, back_grp, residual, blocks, basis, aux_sub, aux_grp)


def advance_body(image_ref, residual_ref, curve_ref, product_ref, residual_out, half_out):
    width = curve_ref.shape[1]
    scale = per_row(product_ref[...] / curve_ref[...], width)
    for b in range(image_ref.shape[1] // width):
        cols = slice(b * width, (b + 1) * width)
        fresh = residual_ref[:, cols] - scale * image_ref[:, cols]
        residual_out[:, cols] = fresh
        half_out[:, cols] = fresh * 0.5


def advance(image, residual, curve, product):
    shape = jax.ShapeDtypeStruct(residual.shape, F32)
    return call(
        advance_body,
        (shape, shape),
        flops=residual.size * 400,
        moved=residual.size * 16,
        in_specs=[VMEM] * 4,
        out_specs=(VMEM,) * 2,
        limit=4 * 1024 * 1024,
    )(image, residual, curve, product)


def first_body(own_ref, sub_ref, grp_ref, curve_ref, product_ref, inverse_ref, coarse_out, first_out):
    scale = per_row(product_ref[...] / curve_ref[...], own_ref.shape[2])
    parts = own_ref[...] + sub_ref[...] + grp_ref[...]
    coarse = parts[1] - scale * parts[0]
    coarse_out[...] = coarse
    first_out[...] = mm3(coarse, inverse_ref[...])


def first_step(own, sub, grp, curve, product, inverse):
    shape = jax.ShapeDtypeStruct(own.shape[1:], F32)
    return call(
        first_body,
        (shape, shape),
        flops=own.size * 128 * 6,
        moved=own.size * 24,
        in_specs=[VMEM] * 6,
        out_specs=(VMEM,) * 2,
        limit=4 * 1024 * 1024,
    )(own, sub, grp, curve, product, inverse)


def merge_body(*refs):
    out_ref = refs[-1]
    for place, ref in enumerate(refs[:-1]):
        size = ref.shape[0]
        out_ref[place * size : (place + 1) * size] = ref[...]


def merge(pieces):
    size = pieces[0].shape[0]
    shape = jax.ShapeDtypeStruct((size * len(pieces),) + pieces[0].shape[1:], F32)
    return call(
        merge_body,
        shape,
        flops=1000,
        moved=shape.size * 8,
        in_specs=[VMEM] * len(pieces),
        out_specs=VMEM,
        limit=4 * 1024 * 1024,
    )(*pieces)


def correct_body(paired, pattern_ref, window_ref, beside_ref, coarse_ref, first_ref, matrix_ref, inverse_ref, local_ref, out_ref, product_ref, held_ref):
    size = window_ref.shape[0]
    held_ref[:size] = window_ref[...]
    held_ref[size:] = beside_ref[...]
    grp_count = lax.axis_size("grp")
    sub_count = lax.axis_size("sub")
    my_sub = lax.axis_index("sub")
    my_grp = lax.axis_index("grp")
    acc = None
    for k in range(matrix_ref.shape[0]):
        entry = pattern_ref[0, k]
        entry_sub = entry // grp_count
        entry_grp = entry - entry_sub * grp_count
        offset = lax.rem(entry_sub - my_sub + REACH_SUBS + sub_count, sub_count) - REACH_SUBS
        position = sub_slot(offset, my_sub, sub_count)
        if paired:
            apart = entry_grp ^ my_grp
            index = ((apart & 1) * (2 * REACH_SUBS + 1) + position) * 2 + (apart >> 1)
        else:
            index = position * grp_count + entry_grp
        term = mm3(held_ref[index], matrix_ref[k])
        acc = term if acc is None else acc + term
    coarse = coarse_ref[...]
    result = first_ref[...] + mm3(coarse - acc, inverse_ref[...])
    out_ref[...] = result
    product_ref[...] = row_sums(coarse * result) + local_ref[...]


def correct(paired, pattern, window, beside, coarse, first, matrix, inverse, local):
    shape = jax.ShapeDtypeStruct(first.shape, F32)
    return call(
        functools.partial(correct_body, paired),
        (shape, jax.ShapeDtypeStruct((8, first.shape[0]), F32)),
        flops=matrix.size * 128 * 6,
        moved=window.size * 4,
        scratch=[pltpu.VMEM((window.shape[0] + beside.shape[0],) + window.shape[1:], F32)],
        in_specs=[SMEM] + [VMEM] * 7,
        out_specs=(VMEM, VMEM),
        limit=8 * 1024 * 1024,
    )(pattern, window, beside, coarse, first, matrix, inverse, local)


def local_body(slots_ref, halved_ref, factor_ref, aux_sub_ref, aux_grp_ref, out_ref, product_ref):
    width = factor_ref.shape[1]
    half = halved_ref.shape[1] // 2
    per_face = half // width
    acc = jnp.zeros((halved_ref.shape[0], width), F32)
    for which, aux in ((1, aux_sub_ref), (3, aux_grp_ref)):
        base = (which // 2) * half
        first = slots_ref[0, which] * per_face
        for b in range(per_face):
            cols = slice(base + b * width, base + (b + 1) * width)
            halved = halved_ref[:, cols]
            high, low = split(halved)
            mine = factor_ref[first + b]
            theirs = aux[b * width : (b + 1) * width, :].astype(BF16)
            pair = jnp.concatenate([mine, theirs], 1)
            middle = mm(jnp.concatenate([high, low], 1), twice(pair, 0))
            middle_high, middle_low = split(middle)
            solved = mm(middle_high, pair, NT) + mm(middle_low, pair, NT)
            out_ref[:, cols] = solved * 0.5
            acc += halved * solved
    product_ref[...] = row_sums(acc)


def local_solve(slots, fresh, factor, aux_sub, aux_grp):
    return call(
        local_body,
        (jax.ShapeDtypeStruct(fresh.shape, F32), jax.ShapeDtypeStruct((8, fresh.shape[0]), F32)),
        flops=fresh.size * 128 * 16,
        moved=fresh.size * 12,
        in_specs=[SMEM] + [VMEM] * 4,
        out_specs=(VMEM, VMEM),
        limit=10 * 1024 * 1024,
    )(slots, fresh, factor, aux_sub, aux_grp)


def spread_body(slots_ref, solved_ref, own_ref, from_sub_ref, from_grp_ref, block_ref, basis_ref, aux_sub_ref, aux_grp_ref, iterate_ref, direction_ref, curve_ref, product_ref, out_ref, iterate_out):
    width = basis_ref.shape[1]
    prims = basis_ref.shape[0]
    half = solved_ref.shape[1] // 2
    per_face = half // width
    rows = half
    own = own_ref[...] * 0.5
    basis = basis_ref[...]
    scale = per_row(product_ref[...] / curve_ref[...], width)
    for which, aux, other_ref in ((1, aux_sub_ref, from_sub_ref), (3, aux_grp_ref, from_grp_ref)):
        base = (which // 2) * half
        both = jnp.concatenate([own, other_ref[...] * 0.5], 1)
        right = jnp.concatenate([basis, aux[rows : rows + prims, :].astype(BF16)], 0)
        own_near = (block_ref[...] - slots_ref[0, which] * per_face).astype(F32)
        near = jnp.concatenate([own_near, aux[rows + prims : rows + prims + 1, :]], 1)
        for b in range(per_face):
            cols = slice(base + b * width, base + (b + 1) * width)
            high, low = split(jnp.where(near == b, both, 0.0))
            out_ref[:, cols] = solved_ref[:, cols] + (mm(high, right) + mm(low, right))
            iterate_out[:, cols] = iterate_ref[:, cols] + scale * direction_ref[:, cols]


def spread(slots, solved, own, from_sub, from_grp, blocks, basis, aux_sub, aux_grp, iterate, direction, curve, product):
    return call(
        spread_body,
        (jax.ShapeDtypeStruct(solved.shape, F32),) * 2,
        flops=solved.size * 128 * 8,
        moved=solved.size * 12,
        in_specs=[SMEM] + [VMEM] * 12,
        out_specs=(VMEM, VMEM),
        limit=10 * 1024 * 1024,
    )(slots, solved, own, from_sub, from_grp, blocks, basis, aux_sub, aux_grp, iterate, direction, curve, product)


def finish_body(made_ref, direction_ref, sum_ref, product_ref, direction_out, sum_out):
    width = sum_ref.shape[1]
    scale = per_row(sum_ref[...] / product_ref[...], width)
    sum_out[...] = sum_ref[0:1]
    for b in range(made_ref.shape[1] // width):
        cols = slice(b * width, (b + 1) * width)
        direction_out[:, cols] = made_ref[:, cols] + scale * direction_ref[:, cols]


def finish(made, direction, total_sum, product):
    return call(
        finish_body,
        (jax.ShapeDtypeStruct(made.shape, F32), jax.ShapeDtypeStruct(product.shape, F32)),
        flops=made.size * 2,
        moved=made.size * 12,
        in_specs=[VMEM] * 4,
        out_specs=(VMEM, VMEM),
        limit=4 * 1024 * 1024,
    )(made, direction, total_sum, product)


def shards(
    solution,
    residual,
    direction,
    residual_product,
    neighbor_slots,
    coupling,
    dirichlet_factor,
    face_block,
    neumann_factor,
    primal_block,
    primal_basis,
    coarse_matrix,
    coarse_block_inverse,
    coarse_pattern,
):
    width = face_block.shape[2]
    per_face = face_block.shape[1] // 4
    face_width = per_face * width
    own = direction[0]
    basis = primal_basis[0]
    factor = neumann_factor[0]
    product = residual_product[None, :]
    grp_count = lax.axis_size("grp")

    from_sub = shifted(own[:, :face_width], "sub", 1)
    from_grp = shifted(own[:, face_width:], "grp", 1)
    keep = (face_block[0], factor, basis, primal_block)
    couple, middle, face, factor, basis, blocks = prepare(coupling[0], dirichlet_factor[0], keep)
    aux_sub, aux_grp = pack(neighbor_slots, blocks, basis, factor, per_face)
    aux_sub, aux_grp, face = lax.optimization_barrier((aux_sub, aux_grp, face))
    aux_sub = shifted(aux_sub, "sub", -1)
    aux_grp = shifted(aux_grp, "grp", -1)
    keep = (own, residual[0], coarse_matrix[0], coarse_block_inverse[0], solution[0])
    high, low, own, old, matrix, inverse, iterate = assemble(couple, middle, face, keep)

    y, curve = apply(neighbor_slots, own, from_sub, from_grp, high, low)
    back_sub = shifted(y[0], "sub", -1)
    curve = total(curve, "grp")
    lower, curve = lax.optimization_barrier((y[2], curve))
    back_grp = shifted(lower, "grp", -1)
    curve = total(curve, "sub")
    image, part, part_sub, part_grp = find_image(
        neighbor_slots, y, back_sub, back_grp, old, blocks, basis, aux_sub, aux_grp
    )
    part_sub = shifted(part_sub, "sub", 1)
    part_grp = shifted(part_grp, "grp", 1)
    coarse, first = first_step(part, part_sub, part_grp, curve, product, inverse)
    fresh, halved = advance(image, old, curve, product)
    solved, local = local_solve(neighbor_slots, halved, factor, aux_sub, aux_grp)

    if grp_count == 4:
        beyond = shifted(first, "grp", 2)
        group = jnp.stack([first, beyond], 0)
    else:
        group = lax.all_gather(first[None], "grp", axis=0, tiled=True)
    window = merge([group] + sub_window(group))
    beside = window[:1]
    if grp_count == 4:
        beside = lax.ppermute(window, "grp", [(i, i ^ 1) for i in range(grp_count)])

    correction, partial = correct(grp_count == 4, coarse_pattern, window, beside, coarse, first, matrix, inverse, local)
    partial = total(partial, "grp")
    sent, partial = lax.optimization_barrier((correction, partial))
    other_sub = shifted(sent, "sub", -1)
    other_grp = shifted(sent, "grp", -1)

    def late(value):
        value, first_in, second_in = lax.optimization_barrier((value, other_sub, other_grp))
        return value, spread(
            neighbor_slots, solved, correction, first_in, second_in, blocks, basis, aux_sub, aux_grp, iterate, own, curve, product
        )

    new_product, (preconditioned, new_solution) = total_with(partial, "sub", late)
    new_direction, new_product = finish(preconditioned, own, new_product, product)
    return (new_solution[None], fresh[None], new_direction[None], new_product[0])


def solution(mesh):
    in_specs = (
        P(("sub", "grp"), None, None),
        P(("sub", "grp"), None, None),
        P(("sub", "grp"), None, None),
        P(),
        P(("sub", "grp"), None),
        P(("sub", "grp"), None, None, None),
        P(("sub", "grp"), None, None, None),
        P(("sub", "grp"), None, None, None),
        P(("sub", "grp"), None, None, None),
        P(("sub", "grp"), None),
        P(("sub", "grp"), None, None),
        P(("sub", "grp"), None, None, None),
        P(("sub", "grp"), None, None),
        P(("sub", "grp"), None),
    )
    out_specs = (
        P(("sub", "grp"), None, None),
        P(("sub", "grp"), None, None),
        P(("sub", "grp"), None, None),
        P(),
    )

    return jax.shard_map(shards, mesh=mesh, in_specs=in_specs, out_specs=out_specs, check_vma=False)
```

```python
import functools

import jax
import jax.numpy as jnp
from jax import lax
from jax.experimental import pallas as pl
from jax.experimental.pallas import tpu as pltpu
from jax.sharding import PartitionSpec as P


REACH_SUBS = 2
F32 = jnp.float32
BF16 = jnp.bfloat16
VMEM = pl.BlockSpec(memory_space=pltpu.VMEM)
SMEM = pl.BlockSpec(memory_space=pltpu.SMEM)
NN = (((1,), (0,)), ((), ()))
NT = (((1,), (1,)), ((), ()))


def shifted(value, axis, steps):
    count = lax.axis_size(axis)
    pairs = [(source, (source + steps) % count) for source in range(count)]
    return lax.ppermute(value, axis, pairs)


def total(value, axis):
    count = lax.axis_size(axis)
    if count & (count - 1):
        return lax.psum(value, axis)
    bits = [1 << k for k in range(count.bit_length() - 1)]
    for bit in reversed(bits) if axis == "sub" else bits:
        value = value + lax.ppermute(value, axis, [(i, i ^ bit) for i in range(count)])
    return value


def total_with(value, axis, late):
    count = lax.axis_size(axis)
    if count & (count - 1):
        value, extra = late(value)
        return lax.psum(value, axis), extra
    bit = 1
    extra = None
    while bit < count:
        if 2 * bit == count:
            value, extra = late(value)
        value = value + lax.ppermute(value, axis, [(i, i ^ bit) for i in range(count)])
        bit *= 2
    return value, extra


def swapped_window(count):
    return REACH_SUBS == 2 and count % 4 == 0 and count > 4


def sub_window(group):
    count = lax.axis_size("sub")
    everyone = range(count)
    if swapped_window(count):
        targets = (
            [i ^ 1 for i in everyone],
            [(i - 1 + 2 * (i & 1)) % count for i in everyone],
            [i ^ 2 for i in everyone],
            [(i - 2 + 2 * (i & 2)) % count for i in everyone],
        )
    else:
        targets = [[(i - step) % count for i in everyone] for step in range(-REACH_SUBS, REACH_SUBS + 1) if step]
    pieces = []
    for target in targets:
        pieces.append(lax.ppermute(group, "sub", list(zip(everyone, target))))
    return pieces


def sub_slot(offset, mine, count):
    if swapped_window(count):
        far = jnp.where((mine & 2 == 0) == (offset == 2), 3, 4)
        near = jnp.where((mine & 1 == 0) == (offset == 1), 1, 2)
        return jnp.where(offset == 0, 0, jnp.where((offset == 1) | (offset == -1), near, far))
    return jnp.where(offset == 0, 0, offset + REACH_SUBS + (offset < 0).astype(jnp.int32))


def split(value):
    high = value.astype(BF16)
    low = (value - high.astype(F32)).astype(BF16)
    return high, low


def mm(a, b, dims=NN):
    return lax.dot_general(a, b, dims, preferred_element_type=F32)


def mm3(a, b):
    a_high, a_low = split(a)
    b_high, b_low = split(b)
    return mm(a_high, b_high) + (mm(a_low, b_high) + mm(a_high, b_low))


def twice(value, axis):
    return jnp.concatenate([value, value], axis=axis)


def row_sums(partial):
    ones = jnp.ones((8, partial.shape[1]), F32)
    return lax.dot_general(ones, partial, NT, precision=lax.Precision.HIGHEST, preferred_element_type=F32)


def per_row(row, width):
    tall = jnp.broadcast_to(row[0:1], (width, row.shape[1]))
    return tall.T


def call(body, out_shapes, flops, moved, scratch=(), grid=None, in_specs=None, out_specs=None, limit=None):
    params = {}
    if limit is not None:
        params["vmem_limit_bytes"] = limit
    kwargs = {}
    if grid is not None:
        kwargs["grid"] = grid
    return pl.pallas_call(
        body,
        out_shape=out_shapes,
        in_specs=in_specs,
        out_specs=out_specs,
        scratch_shapes=scratch,
        compiler_params=pltpu.CompilerParams(**params),
        cost_estimate=pl.CostEstimate(flops=flops, bytes_accessed=moved, transcendentals=0),
        **kwargs,
    )


BATCH = 16
LAST_BATCH = 32


def in_hbm(value):
    return pltpu.with_memory_space_constraint(value, pltpu.HBM)


def prepare_body(kept, couple_hbm, factor_hbm, *refs):
    sources = refs[:kept]
    couple_ref, middle_ref = refs[kept : kept + 2]
    targets = refs[kept + 2 : 2 * kept + 2]
    factor_ref, inner_ref, sems, keep_sems = refs[2 * kept + 2 :]
    width = factor_ref.shape[1]
    rounds = couple_ref.shape[0] // BATCH

    def copy_of(i, which):
        part = pl.ds(i * BATCH, BATCH)
        source, target = ((factor_hbm, factor_ref), (couple_hbm, couple_ref))[which]
        return pltpu.make_async_copy(source.at[part], target.at[part], sems.at[which, i])

    def begin(i, carry):
        for which in range(2):
            copy_of(i, which).start()
        return carry

    keeping = [pltpu.make_async_copy(a, b, keep_sems.at[i]) for i, (a, b) in enumerate(zip(sources, targets))]
    lax.fori_loop(0, rounds, begin, 0)
    for copy in keeping:
        copy.start()

    def inner(i):
        for k in range(BATCH):
            factor = factor_ref[i * BATCH + k]
            high, low = split(mm(factor, factor, NT))
            inner_ref[i % 2, k, :width] = high
            inner_ref[i % 2, k, width:] = low

    def middle(i):
        for k in range(BATCH):
            high, low = split(mm(twice(couple_ref[i * BATCH + k], 1), inner_ref[i % 2, k]))
            middle_ref[i * BATCH + k, :, :width] = high
            middle_ref[i * BATCH + k, :, width:] = low

    copy_of(0, 0).wait()
    inner(0)

    def steady(i, carry):
        copy_of(i, 0).wait()
        copy_of(i - 1, 1).wait()
        inner(i)
        middle(i - 1)
        return carry

    lax.fori_loop(1, rounds, steady, 0)
    copy_of(rounds - 1, 1).wait()
    middle(rounds - 1)
    for copy in keeping:
        copy.wait()


def prepare(coupling, dirichlet, keep):
    count, double, width = coupling.shape
    hbm = pl.BlockSpec(memory_space=pltpu.HBM)
    return call(
        functools.partial(prepare_body, len(keep)),
        (
            jax.ShapeDtypeStruct(coupling.shape, BF16),
            jax.ShapeDtypeStruct((count, double, double), BF16),
        )
        + tuple(jax.ShapeDtypeStruct(k.shape, k.dtype) for k in keep),
        flops=count * 2 * width**3 * 6,
        moved=coupling.size * 3,
        scratch=[
            pltpu.VMEM((count, width, width), BF16),
            pltpu.VMEM((2, BATCH, double, width), BF16),
            pltpu.SemaphoreType.DMA((2, count // BATCH)),
            pltpu.SemaphoreType.DMA((len(keep),)),
        ],
        in_specs=[hbm] * (2 + len(keep)),
        out_specs=(VMEM,) * (2 + len(keep)),
        limit=6 * 1024 * 1024,
    )(in_hbm(coupling), in_hbm(dirichlet), *(in_hbm(k) for k in keep))


def assemble_body(blocks, kept, couple_ref, middle_ref, face_ref, *refs):
    sources = refs[:kept]
    high_ref, low_ref = refs[kept : kept + 2]
    targets = refs[kept + 2 : 2 * kept + 2]
    near_ref, far_ref, keep_sems = refs[2 * kept + 2 :]
    width = face_ref.shape[1]
    count = couple_ref.shape[0]
    reach = count // blocks
    pairs = blocks // 2
    keeping = [pltpu.make_async_copy(a, b, keep_sems.at[i]) for i, (a, b) in enumerate(zip(sources, targets))]
    for copy in keeping:
        copy.start()

    def convert(block, carry):
        near_ref[block] = face_ref[block].astype(F32)
        far_ref[block] = jnp.zeros((width, width), F32)
        return carry

    lax.fori_loop(0, blocks, convert, 0)
    for extra in range(reach):
        far_ref[blocks + extra] = jnp.zeros((width, width), F32)

    def put(pair, row, half, value):
        high, low = split(value)
        cols = pl.ds(pl.multiple_of(half * width, width), width)
        high_ref[pair, row, :, cols] = high
        low_ref[pair, row, :, cols] = low

    def outer(i, carry):
        per = blocks // LAST_BATCH
        q = i // per
        base = (i - q * per) * LAST_BATCH
        for k in range(LAST_BATCH):
            full = mm(middle_ref[i * LAST_BATCH + k], twice(couple_ref[i * LAST_BATCH + k], 1), NT)
            place = base + k
            reached = place + q + 1
            near_ref[place] += full[:width, :width]
            far_ref[reached] += full[width:, width:]
            wrapped = lax.rem(reached, blocks)
            half = lax.rem(wrapped, 2)
            put(wrapped // 2, reach - 1 - q + half, half, full[:width, width:])
            side = k % 2
            put(place // 2, reach + q + 1 + side, side, full[width:, :width])
        return carry

    lax.fori_loop(0, count // LAST_BATCH, outer, 0)

    def close(pair, carry):
        zero = jnp.zeros((width, width), BF16)
        for ref in (high_ref, low_ref):
            ref[pair, 2 * reach + 1, :, pl.ds(0, width)] = zero
            ref[pair, 0, :, pl.ds(width, width)] = zero
        for side in range(2):
            put(pair, reach + side, side, near_ref[2 * pair + side] + far_ref[2 * pair + side])
        return carry

    for extra in range(reach):
        far_ref[extra] += far_ref[blocks + extra]
    lax.fori_loop(0, pairs, close, 0)
    for copy in keeping:
        copy.wait()


def assemble(couple, middle, face, keep):
    blocks, width, _ = face.shape
    count = couple.shape[0]
    reach = count // blocks
    pairs = blocks // 2
    shape = jax.ShapeDtypeStruct((pairs, 2 * reach + 2, width, 2 * width), BF16)
    hbm = pl.BlockSpec(memory_space=pltpu.HBM)
    return call(
        functools.partial(assemble_body, blocks, len(keep)),
        (shape, shape) + tuple(jax.ShapeDtypeStruct(k.shape, k.dtype) for k in keep),
        flops=count * 2 * width**3 * 6,
        moved=couple.size * 3,
        scratch=[
            pltpu.VMEM((blocks, width, width), F32),
            pltpu.VMEM((blocks + reach, width, width), F32),
            pltpu.SemaphoreType.DMA((len(keep),)),
        ],
        in_specs=[VMEM] * 3 + [hbm] * len(keep),
        out_specs=(VMEM,) * (2 + len(keep)),
        limit=6 * 1024 * 1024,
    )(couple, middle, face, *(in_hbm(k) for k in keep))


def one_face(which, slots_ref, face, base, high_ref, low_ref, u_high, u_low, out_ref, acc):
    _, count, width, _ = high_ref.shape
    loads, face_width = out_ref.shape
    half_face = face_width // width // 2
    slot = slots_ref[0, which]
    for part in range(half_face):
        pair = slot * half_face + part
        high = jnp.concatenate([u_high[2 * pair + i] for i in range(count)], 1)
        low = jnp.concatenate([u_low[2 * pair + i] for i in range(count)], 1)
        weight = high_ref[pair].reshape(count * width, 2 * width)
        both = mm(jnp.concatenate([high, low], 0), weight)
        result = both[:loads] + both[loads:] + mm(high, low_ref[pair].reshape(count * width, 2 * width))
        first = 2 * part * width
        out_ref[:, first : first + 2 * width] = result
        acc += face[:, base + first : base + first + width] * result[:, :width]
        acc += face[:, base + first + width : base + first + 2 * width] * result[:, width:]
    return acc


def apply_body(slots_ref, own_ref, from_sub_ref, from_grp_ref, high_ref, low_ref, sub_out, grp_out, acc_out, u_high, u_low):
    pairs, count, width, _ = high_ref.shape
    reach = count // 2 - 1
    face_width = from_sub_ref.shape[1]
    per_face = face_width // width
    blocks = 2 * pairs
    loads = own_ref.shape[0]
    faces = ((from_sub_ref, 0), (own_ref, 0), (from_grp_ref, 0), (own_ref, face_width))
    for which, (ref, base) in enumerate(faces):
        slot = slots_ref[0, which]
        for b in range(per_face):
            high, low = split(ref[:, base + b * width : base + (b + 1) * width])
            place = slot * per_face + b + reach
            u_high[place] = high
            u_low[place] = low
    for ref in (u_high, u_low):
        for i in range(reach):
            ref[i] = ref[blocks + i]
        for i in range(reach + 1):
            ref[blocks + reach + i] = ref[reach + i]
    acc = jnp.zeros((loads, width), F32)
    acc = one_face(0, slots_ref, from_sub_ref, 0, high_ref, low_ref, u_high, u_low, sub_out, acc)
    acc_out[...] = one_face(2, slots_ref, from_grp_ref, 0, high_ref, low_ref, u_high, u_low, grp_out, acc)


def apply(slots, own, from_sub, from_grp, high, low):
    pairs, count, width, _ = high.shape
    loads, face_width = from_sub.shape
    face = jax.ShapeDtypeStruct((loads, face_width), F32)
    kept = jax.ShapeDtypeStruct((2 * pairs + count - 1, loads, width), BF16)
    return call(
        apply_body,
        (face, face, jax.ShapeDtypeStruct((loads, width), F32), kept, kept),
        flops=high.size * loads * 3,
        moved=high.size * 4,
        in_specs=[SMEM] + [VMEM] * 5,
        out_specs=(VMEM,) * 5,
        limit=6 * 1024 * 1024,
    )(slots, own, from_sub, from_grp, high, low)


def rest_body(slots_ref, own_ref, acc_ref, u_high, u_low, high_ref, low_ref, sub_out, grp_out, curve_ref):
    face_width = sub_out.shape[1]
    acc = one_face(1, slots_ref, own_ref, 0, high_ref, low_ref, u_high, u_low, sub_out, acc_ref[...])
    acc = one_face(3, slots_ref, own_ref, face_width, high_ref, low_ref, u_high, u_low, grp_out, acc)
    curve_ref[...] = row_sums(acc)


def apply_rest(slots, own, acc, u_high, u_low, high, low):
    loads = own.shape[0]
    face = jax.ShapeDtypeStruct((loads, own.shape[1] // 2), F32)
    return call(
        rest_body,
        (face, face, jax.ShapeDtypeStruct((8, loads), F32)),
        flops=high.size * loads * 3,
        moved=high.size * 4,
        in_specs=[SMEM] + [VMEM] * 6,
        out_specs=(VMEM,) * 3,
        limit=6 * 1024 * 1024,
    )(slots, own, acc, u_high, u_low, high, low)


def pack_body(per_face, slots_ref, block_ref, basis_ref, factor_ref, sub_ref, grp_ref):
    prims, width = basis_ref.shape
    rows = per_face * width
    for out, which in ((sub_ref, 0), (grp_ref, 2)):
        first = slots_ref[0, which] * per_face
        for b in range(per_face):
            out[b * width : (b + 1) * width, :] = factor_ref[first + b].astype(F32)
        out[rows : rows + prims, :] = basis_ref[...].astype(F32)
        near = (block_ref[...] - first).astype(F32)
        out[rows + prims :, :] = jnp.broadcast_to(near, (8, width))


def pack(slots, blocks, basis, factor, per_face):
    prims, width = basis.shape
    shape = jax.ShapeDtypeStruct((per_face * width + prims + 8, width), F32)
    return call(
        functools.partial(pack_body, per_face),
        (shape, shape),
        flops=1000,
        moved=shape.size * 12,
        in_specs=[SMEM] + [VMEM] * 3,
        out_specs=(VMEM, VMEM),
        limit=4 * 1024 * 1024,
    )(slots, blocks, basis, factor)


def image_body(slots_ref, y_sub_ref, y_grp_ref, back_sub_ref, back_grp_ref, residual_ref, block_ref, basis_ref, aux_sub_ref, aux_grp_ref, image_out, own_out, sub_out, grp_out):
    prims, width = basis_ref.shape
    face_width = back_sub_ref.shape[1]
    per_face = face_width // width
    rows = face_width
    loads = residual_ref.shape[0]
    basis = basis_ref[...].astype(F32).T
    own_total = None
    for which, y_ref, back, aux, out in (
        (1, y_sub_ref, back_sub_ref, aux_sub_ref, sub_out),
        (3, y_grp_ref, back_grp_ref, aux_grp_ref, grp_out),
    ):
        offset = (which // 2) * face_width
        other = aux[rows : rows + prims, :].T
        own_near = block_ref[...] - slots_ref[0, which] * per_face
        other_near = aux[rows + prims : rows + prims + 1, :]
        both = None
        for b in range(per_face):
            cols = slice(b * width, (b + 1) * width)
            wide = slice(offset + b * width, offset + (b + 1) * width)
            image = y_ref[:, cols] + back[:, cols]
            image_out[:, wide] = image
            image_high, image_low = split(image)
            high, low = split(residual_ref[:, wide])
            left = jnp.concatenate(
                [jnp.concatenate([image_high, image_low], 1), jnp.concatenate([high, low], 1)], 0
            )
            mine = jnp.where(own_near == b, basis, 0.0).astype(BF16)
            theirs = jnp.where(other_near == b, other, 0.0).astype(BF16)
            term = mm(left, twice(jnp.concatenate([mine, theirs], 1), 0))
            both = term if both is None else both + term
        own = both[:, :prims]
        own_total = own if own_total is None else own_total + own
        out[0] = both[:loads, prims:] * 0.5
        out[1] = both[loads:, prims:] * 0.5
    own_out[0] = own_total[:loads] * 0.5
    own_out[1] = own_total[loads:] * 0.5


def find_image(slots, y_sub, y_grp, back_sub, back_grp, residual, blocks, basis, aux_sub, aux_grp):
    loads = residual.shape[0]
    prims = basis.shape[0]
    small = jax.ShapeDtypeStruct((2, loads, prims), F32)
    return call(
        image_body,
        (jax.ShapeDtypeStruct(residual.shape, F32), small, small, small),
        flops=residual.size * prims * 16,
        moved=residual.size * 20,
        in_specs=[SMEM] + [VMEM] * 9,
        out_specs=(VMEM,) * 4,
        limit=8 * 1024 * 1024,
    )(slots, y_sub, y_grp, back_sub, back_grp, residual, blocks, basis, aux_sub, aux_grp)


def advance_body(image_ref, residual_ref, curve_ref, product_ref, residual_out, half_out):
    width = curve_ref.shape[1]
    scale = per_row(product_ref[...] / curve_ref[...], width)
    for b in range(image_ref.shape[1] // width):
        cols = slice(b * width, (b + 1) * width)
        fresh = residual_ref[:, cols] - scale * image_ref[:, cols]
        residual_out[:, cols] = fresh
        half_out[:, cols] = fresh * 0.5


def advance(image, residual, curve, product):
    shape = jax.ShapeDtypeStruct(residual.shape, F32)
    return call(
        advance_body,
        (shape, shape),
        flops=residual.size * 400,
        moved=residual.size * 16,
        in_specs=[VMEM] * 4,
        out_specs=(VMEM,) * 2,
        limit=4 * 1024 * 1024,
    )(image, residual, curve, product)


def first_body(own_ref, sub_ref, grp_ref, curve_ref, product_ref, inverse_ref, coarse_out, first_out):
    scale = per_row(product_ref[...] / curve_ref[...], own_ref.shape[2])
    parts = own_ref[...] + sub_ref[...] + grp_ref[...]
    coarse = parts[1] - scale * parts[0]
    coarse_out[...] = coarse
    first_out[...] = mm3(coarse, inverse_ref[...])


def first_step(own, sub, grp, curve, product, inverse):
    shape = jax.ShapeDtypeStruct(own.shape[1:], F32)
    return call(
        first_body,
        (shape, shape),
        flops=own.size * 128 * 6,
        moved=own.size * 24,
        in_specs=[VMEM] * 6,
        out_specs=(VMEM,) * 2,
        limit=4 * 1024 * 1024,
    )(own, sub, grp, curve, product, inverse)


def merge_body(*refs):
    out_ref = refs[-1]
    for place, ref in enumerate(refs[:-1]):
        size = ref.shape[0]
        out_ref[place * size : (place + 1) * size] = ref[...]


def merge(pieces):
    size = pieces[0].shape[0]
    shape = jax.ShapeDtypeStruct((size * len(pieces),) + pieces[0].shape[1:], F32)
    return call(
        merge_body,
        shape,
        flops=1000,
        moved=shape.size * 8,
        in_specs=[VMEM] * len(pieces),
        out_specs=VMEM,
        limit=4 * 1024 * 1024,
    )(*pieces)


def correct_body(paired, pattern_ref, window_ref, beside_ref, coarse_ref, first_ref, matrix_ref, inverse_ref, local_ref, out_ref, product_ref, held_ref):
    size = window_ref.shape[0]
    held_ref[:size] = window_ref[...]
    held_ref[size:] = beside_ref[...]
    grp_count = lax.axis_size("grp")
    sub_count = lax.axis_size("sub")
    my_sub = lax.axis_index("sub")
    my_grp = lax.axis_index("grp")
    acc = None
    for k in range(matrix_ref.shape[0]):
        entry = pattern_ref[0, k]
        entry_sub = entry // grp_count
        entry_grp = entry - entry_sub * grp_count
        offset = lax.rem(entry_sub - my_sub + REACH_SUBS + sub_count, sub_count) - REACH_SUBS
        position = sub_slot(offset, my_sub, sub_count)
        if paired:
            apart = entry_grp ^ my_grp
            index = ((apart & 1) * (2 * REACH_SUBS + 1) + position) * 2 + (apart >> 1)
        else:
            index = position * grp_count + entry_grp
        term = mm3(held_ref[index], matrix_ref[k])
        acc = term if acc is None else acc + term
    coarse = coarse_ref[...]
    result = first_ref[...] + mm3(coarse - acc, inverse_ref[...])
    out_ref[...] = result
    product_ref[...] = row_sums(coarse * result) + local_ref[...]


def correct(paired, pattern, window, beside, coarse, first, matrix, inverse, local):
    shape = jax.ShapeDtypeStruct(first.shape, F32)
    return call(
        functools.partial(correct_body, paired),
        (shape, jax.ShapeDtypeStruct((8, first.shape[0]), F32)),
        flops=matrix.size * 128 * 6,
        moved=window.size * 4,
        scratch=[pltpu.VMEM((window.shape[0] + beside.shape[0],) + window.shape[1:], F32)],
        in_specs=[SMEM] + [VMEM] * 7,
        out_specs=(VMEM, VMEM),
        limit=8 * 1024 * 1024,
    )(pattern, window, beside, coarse, first, matrix, inverse, local)


def local_body(slots_ref, halved_ref, factor_ref, aux_sub_ref, aux_grp_ref, out_ref, product_ref):
    width = factor_ref.shape[1]
    half = halved_ref.shape[1] // 2
    per_face = half // width
    acc = jnp.zeros((halved_ref.shape[0], width), F32)
    for which, aux in ((1, aux_sub_ref), (3, aux_grp_ref)):
        base = (which // 2) * half
        first = slots_ref[0, which] * per_face
        for b in range(per_face):
            cols = slice(base + b * width, base + (b + 1) * width)
            halved = halved_ref[:, cols]
            high, low = split(halved)
            mine = factor_ref[first + b]
            theirs = aux[b * width : (b + 1) * width, :].astype(BF16)
            pair = jnp.concatenate([mine, theirs], 1)
            middle = mm(jnp.concatenate([high, low], 1), twice(pair, 0))
            middle_high, middle_low = split(middle)
            solved = mm(middle_high, pair, NT) + mm(middle_low, pair, NT)
            out_ref[:, cols] = solved * 0.5
            acc += halved * solved
    product_ref[...] = row_sums(acc)


def local_solve(slots, fresh, factor, aux_sub, aux_grp):
    return call(
        local_body,
        (jax.ShapeDtypeStruct(fresh.shape, F32), jax.ShapeDtypeStruct((8, fresh.shape[0]), F32)),
        flops=fresh.size * 128 * 16,
        moved=fresh.size * 12,
        in_specs=[SMEM] + [VMEM] * 4,
        out_specs=(VMEM, VMEM),
        limit=10 * 1024 * 1024,
    )(slots, fresh, factor, aux_sub, aux_grp)


def spread_body(slots_ref, solved_ref, own_ref, from_sub_ref, from_grp_ref, block_ref, basis_ref, aux_sub_ref, aux_grp_ref, iterate_ref, direction_ref, curve_ref, product_ref, out_ref, iterate_out):
    width = basis_ref.shape[1]
    prims = basis_ref.shape[0]
    half = solved_ref.shape[1] // 2
    per_face = half // width
    rows = half
    own = own_ref[...] * 0.5
    basis = basis_ref[...]
    scale = per_row(product_ref[...] / curve_ref[...], width)
    for which, aux, other_ref in ((1, aux_sub_ref, from_sub_ref), (3, aux_grp_ref, from_grp_ref)):
        base = (which // 2) * half
        both = jnp.concatenate([own, other_ref[...] * 0.5], 1)
        right = jnp.concatenate([basis, aux[rows : rows + prims, :].astype(BF16)], 0)
        own_near = (block_ref[...] - slots_ref[0, which] * per_face).astype(F32)
        near = jnp.concatenate([own_near, aux[rows + prims : rows + prims + 1, :]], 1)
        for b in range(per_face):
            cols = slice(base + b * width, base + (b + 1) * width)
            high, low = split(jnp.where(near == b, both, 0.0))
            out_ref[:, cols] = solved_ref[:, cols] + (mm(high, right) + mm(low, right))
            iterate_out[:, cols] = iterate_ref[:, cols] + scale * direction_ref[:, cols]


def spread(slots, solved, own, from_sub, from_grp, blocks, basis, aux_sub, aux_grp, iterate, direction, curve, product):
    return call(
        spread_body,
        (jax.ShapeDtypeStruct(solved.shape, F32),) * 2,
        flops=solved.size * 128 * 8,
        moved=solved.size * 12,
        in_specs=[SMEM] + [VMEM] * 12,
        out_specs=(VMEM, VMEM),
        limit=10 * 1024 * 1024,
    )(slots, solved, own, from_sub, from_grp, blocks, basis, aux_sub, aux_grp, iterate, direction, curve, product)


def finish_body(made_ref, direction_ref, sum_ref, product_ref, direction_out, sum_out):
    width = sum_ref.shape[1]
    scale = per_row(sum_ref[...] / product_ref[...], width)
    sum_out[...] = sum_ref[0:1]
    for b in range(made_ref.shape[1] // width):
        cols = slice(b * width, (b + 1) * width)
        direction_out[:, cols] = made_ref[:, cols] + scale * direction_ref[:, cols]


def finish(made, direction, total_sum, product):
    return call(
        finish_body,
        (jax.ShapeDtypeStruct(made.shape, F32), jax.ShapeDtypeStruct(product.shape, F32)),
        flops=made.size * 2,
        moved=made.size * 12,
        in_specs=[VMEM] * 4,
        out_specs=(VMEM, VMEM),
        limit=4 * 1024 * 1024,
    )(made, direction, total_sum, product)


def shards(
    solution,
    residual,
    direction,
    residual_product,
    neighbor_slots,
    coupling,
    dirichlet_factor,
    face_block,
    neumann_factor,
    primal_block,
    primal_basis,
    coarse_matrix,
    coarse_block_inverse,
    coarse_pattern,
):
    width = face_block.shape[2]
    per_face = face_block.shape[1] // 4
    face_width = per_face * width
    own = direction[0]
    basis = primal_basis[0]
    factor = neumann_factor[0]
    product = residual_product[None, :]
    grp_count = lax.axis_size("grp")

    from_sub = shifted(own[:, :face_width], "sub", 1)
    from_grp = shifted(own[:, face_width:], "grp", 1)
    keep = (face_block[0], factor, basis, primal_block)
    couple, middle, face, factor, basis, blocks = prepare(coupling[0], dirichlet_factor[0], keep)
    aux_sub, aux_grp = pack(neighbor_slots, blocks, basis, factor, per_face)
    aux_sub, aux_grp, face = lax.optimization_barrier((aux_sub, aux_grp, face))
    aux_sub = shifted(aux_sub, "sub", -1)
    aux_grp = shifted(aux_grp, "grp", -1)
    keep = (own, residual[0], coarse_matrix[0], coarse_block_inverse[0], solution[0])
    high, low, own, old, matrix, inverse, iterate = assemble(couple, middle, face, keep)

    y_sub, y_grp, acc, u_high, u_low = apply(neighbor_slots, own, from_sub, from_grp, high, low)
    back_sub = shifted(y_sub, "sub", -1)
    y_sub, kept, curve = apply_rest(neighbor_slots, own, acc, u_high, u_low, high, low)
    back_grp = shifted(y_grp, "grp", -1)
    curve = total(curve, "grp")
    curve = total(curve, "sub")
    image, part, part_sub, part_grp = find_image(
        neighbor_slots, y_sub, kept, back_sub, back_grp, old, blocks, basis, aux_sub, aux_grp
    )
    part_sub = shifted(part_sub, "sub", 1)
    part_grp = shifted(part_grp, "grp", 1)
    coarse, first = first_step(part, part_sub, part_grp, curve, product, inverse)
    fresh, halved = advance(image, old, curve, product)
    solved, local = local_solve(neighbor_slots, halved, factor, aux_sub, aux_grp)

    if grp_count == 4:
        beyond = shifted(first, "grp", 2)
        group = jnp.stack([first, beyond], 0)
    else:
        group = lax.all_gather(first[None], "grp", axis=0, tiled=True)
    window = merge([group] + sub_window(group))
    beside = window[:1]
    if grp_count == 4:
        beside = lax.ppermute(window, "grp", [(i, i ^ 1) for i in range(grp_count)])

    correction, partial = correct(grp_count == 4, coarse_pattern, window, beside, coarse, first, matrix, inverse, local)
    partial = total(partial, "grp")
    sent, partial = lax.optimization_barrier((correction, partial))
    other_sub = shifted(sent, "sub", -1)
    other_grp = shifted(sent, "grp", -1)

    def late(value):
        value, first_in, second_in = lax.optimization_barrier((value, other_sub, other_grp))
        return value, spread(
            neighbor_slots, solved, correction, first_in, second_in, blocks, basis, aux_sub, aux_grp, iterate, own, curve, product
        )

    new_product, (preconditioned, new_solution) = total_with(partial, "sub", late)
    new_direction, new_product = finish(preconditioned, own, new_product, product)
    return (new_solution[None], fresh[None], new_direction[None], new_product[0])


def solution(mesh):
    in_specs = (
        P(("sub", "grp"), None, None),
        P(("sub", "grp"), None, None),
        P(("sub", "grp"), None, None),
        P(),
        P(("sub", "grp"), None),
        P(("sub", "grp"), None, None, None),
        P(("sub", "grp"), None, None, None),
        P(("sub", "grp"), None, None, None),
        P(("sub", "grp"), None, None, None),
        P(("sub", "grp"), None),
        P(("sub", "grp"), None, None),
        P(("sub", "grp"), None, None, None),
        P(("sub", "grp"), None, None),
        P(("sub", "grp"), None),
    )
    out_specs = (
        P(("sub", "grp"), None, None),
        P(("sub", "grp"), None, None),
        P(("sub", "grp"), None, None),
        P(),
    )

    return jax.shard_map(shards, mesh=mesh, in_specs=in_specs, out_specs=out_specs, check_vma=False)
```
